128 devices in a mesh: seq: 8 (over z, y_hi), var: 16 (over y_lo, x, core).
Axes of the slice: x: 4, y: 4 (y_hi: 2, y_lo: 2; y = y_hi * 2 + y_lo), z: 4, core: 2. Of those that a mesh axis runs over, the one named last changes fastest.
Arguments:
- fields: float32 [48, 16, 1, 2048], P('var', None, None, 'seq'), may hold values from -6 to 6
- channel_ids: int32 [48], P('var'), may hold values from 0 to 47, each once
- lead_index: int32 [1], replicated, may hold values from 0 to 14
- embed_weight: bfloat16 [48, 16, 1024], P('var'), may hold values from -2 to 2
- var_table: bfloat16 [48, 1024], replicated, may hold values from -6 to 6
- agg_query: bfloat16 [16, 64], replicated, may hold values from -6 to 6
- agg_kv: bfloat16 [1024, 2, 1024], replicated, may hold values from -1 to 1
- agg_out: bfloat16 [1024, 1024], replicated, may hold values from -1 to 1
- agg_temp: float32 [16], replicated, may hold values from 2 to 8
- pos_table: bfloat16 [2048, 1024], P('seq'), may hold values from -6 to 6
- lead_table: bfloat16 [16, 1024], replicated, may hold values from -6 to 6
- norm_gain: float32 [2, 2, 1024], replicated, may hold values from 0.25 to 1.75
- qkv_weight: bfloat16 [2, 1024, 16, 192], P(None, None, 'var'), may hold values from -0.1875 to 0.1875
- attn_temp: float32 [2, 16], P(None, 'var'), may hold values from 2 to 8
- out_weight: bfloat16 [2, 16, 64, 1024], P(None, 'var'), may hold values from -0.1875 to 0.1875
- up_weight: bfloat16 [2, 1024, 4096], P(None, None, 'var'), may hold values from -0.1875 to 0.1875
- down_weight: bfloat16 [2, 4096, 1024], P(None, 'var'), may hold values from -0.09375 to 0.09375
- final_gain: float32 [1024], replicated, may hold values from 0.25 to 1.75
- head_weight: bfloat16 [1024, 48, 16], replicated, may hold values from -1 to 1
Outputs:
- forecast: float32 [2, 48, 16, 1, 2048], P(None, 'var', None, None, 'seq')
The draws below stay inside these ranges and needn't reach their ends.
Inputs may be any that keep to these rules, and one draw needn't show every extreme that they name: `channel_ids`: each channel names its own row of var_table, every row once. lead_index + 1 names a row of lead_table.
All inputs are finite; a program needn't handle non-finite values.
Results may differ from the reference program's by a relative error of at most 0.006.
Values may be sent and summed in bfloat16 or wider, within the bound.
A program may use at most 128 MiB of HBM per device.

```python
import math
import jax
import jax.numpy as jnp
from jax import lax

VARS = 48
D = 1024
HEADS = 16
CHANNEL_WIDTH = 64
FF = 4096
PIX = 16
PATCHES = 2048
LEADS = 16
LAYERS = 2
STEPS = 2
BATCH = 1


def spread_draw(key, shape, deviation, clip_at):
    values = jnp.clip(jax.random.normal(key, shape, jnp.float32) * deviation, -clip_at, clip_at)
    return values


def draw_fields(key, part):
    return spread_draw(jax.random.fold_in(key, 11), (VARS, PIX, BATCH, PATCHES), 1.0, 6.0)


def draw_embed_weight(key, part):
    deviation = 1.0 / PIX ** 0.5
    return spread_draw(jax.random.fold_in(key, 12), (VARS, PIX, D), deviation, 2.0).astype(jnp.bfloat16)


def draw_agg_kv(key, part):
    deviation = 1.0 / D ** 0.5
    return spread_draw(jax.random.fold_in(key, 13), (D, 2, D), deviation, 1.0).astype(jnp.bfloat16)


def draw_agg_out(key, part):
    deviation = 1.0 / D ** 0.5
    return spread_draw(jax.random.fold_in(key, 14), (D, D), deviation, 1.0).astype(jnp.bfloat16)


def draw_head_weight(key, part):
    deviation = 1.0 / D ** 0.5
    return spread_draw(jax.random.fold_in(key, 15), (D, VARS, PIX), deviation, 1.0).astype(jnp.bfloat16)


def block_levels(own_key, dims, split, smallest, top_value):
    level = 1.0
    for position, shards_of in split:
        heights = jax.random.uniform(jax.random.fold_in(jax.random.fold_in(own_key, 6), position), (shards_of,), jnp.float32, smallest / len(split), top_value / len(split))
        level = level * jnp.repeat(jnp.exp(heights), dims[position] // shards_of).reshape((-1,) + (1,) * (len(dims) - 1 - position))
    return level


def centred(own_key, extent, scale, limit, split=(), kind=jnp.bfloat16):
    loudness = block_levels(own_key, extent, split, -0.22, 0.18) if split else 1.0
    array = jax.random.normal(own_key, extent, jnp.float32) * scale * loudness
    return jnp.minimum(jnp.maximum(array, -limit), limit).astype(kind)


def setup_inputs(seed: int = 0) -> dict:
    key_of = jax.random.split(jax.random.key(seed), 20)
    fields = draw_fields(jax.random.fold_in(key_of[19], 71), 0)
    channel_ids = jax.random.permutation(key_of[1], VARS).astype(jnp.int32)
    lead_index = jax.random.randint(key_of[2], (BATCH,), 0, LEADS - STEPS + 1).astype(jnp.int32)
    embed_weight = draw_embed_weight(jax.random.fold_in(key_of[19], 71), 0)
    var_table = centred(key_of[4], (VARS, D), 1.0, 6.0)
    agg_query = centred(key_of[5], (HEADS, CHANNEL_WIDTH), 1.0, 6.0)
    agg_kv = draw_agg_kv(jax.random.fold_in(key_of[19], 71), 0)
    agg_out = draw_agg_out(jax.random.fold_in(key_of[19], 71), 0)
    agg_temp = jnp.clip(jnp.exp(jax.random.uniform(key_of[8], (HEADS,), jnp.float32, math.log(2.0), math.log(8.0))), 2.0, 8.0)
    pos_table = centred(key_of[9], (PATCHES, D), 1.0, 6.0, ((0, 8),))
    lead_table = centred(key_of[10], (LEADS, D), 1.0, 6.0)
    norm_gain = jnp.clip(1.0 + 0.15 * jax.random.normal(key_of[11], (LAYERS, 2, D), jnp.float32), 0.25, 1.75)
    qkv_weight = centred(key_of[12], (LAYERS, D, HEADS, 3 * CHANNEL_WIDTH), D ** -0.5, 0.1875, ((2, 16),))
    attn_temp = jnp.clip(jnp.exp(math.log(8.0) - 1.3862944 * jax.random.uniform(key_of[13], (LAYERS, HEADS), jnp.float32) ** block_levels(key_of[13], (LAYERS, HEADS), ((1, 16),), -0.2, 0.2)), 2.0, 8.0)
    out_weight = centred(key_of[14], (LAYERS, HEADS, CHANNEL_WIDTH, D), D ** -0.5, 0.1875, ((1, 16),))
    up_weight = centred(key_of[15], (LAYERS, D, FF), D ** -0.5, 0.1875, ((2, 16),))
    down_weight = centred(key_of[16], (LAYERS, FF, D), FF ** -0.5, 0.09375, ((1, 16),))
    final_gain = jnp.clip(1.0 + 0.15 * jax.random.normal(key_of[17], (D,), jnp.float32), 0.25, 1.75)
    head_weight = draw_head_weight(jax.random.fold_in(key_of[19], 71), 0)
    return dict(fields=fields, channel_ids=channel_ids, lead_index=lead_index, embed_weight=embed_weight, var_table=var_table, agg_query=agg_query, agg_kv=agg_kv, agg_out=agg_out, agg_temp=agg_temp, pos_table=pos_table, lead_table=lead_table, norm_gain=norm_gain, qkv_weight=qkv_weight, attn_temp=attn_temp, out_weight=out_weight, up_weight=up_weight, down_weight=down_weight, final_gain=final_gain, head_weight=head_weight)


EPS_NORM = 1e-05
EPS_UNIT = 1e-06

def unit_rows(values):
    return values * lax.rsqrt(lax.optimization_barrier(jnp.mean(values * values, axis=-1, keepdims=True)) + EPS_UNIT)

def layer_norm(values, gain):
    centre = values - lax.optimization_barrier(jnp.mean(values, axis=-1, keepdims=True))
    spread = lax.optimization_barrier(jnp.mean(centre * centre, axis=-1, keepdims=True))
    return centre * lax.rsqrt(spread + EPS_NORM) * gain

def rounded_value(values):
    return lax.optimization_barrier(values.astype(jnp.bfloat16))

def reference(fields, channel_ids, lead_index, embed_weight, var_table, agg_query, agg_kv, agg_out, agg_temp, pos_table, lead_table, norm_gain, qkv_weight, attn_temp, out_weight, up_weight, down_weight, final_gain, head_weight):
    rows_all = BATCH * PATCHES
    ident_vars = (channel_ids[:, None] == jnp.arange(VARS, dtype=jnp.int32)[None, :]).astype(jnp.bfloat16)
    var_rows = jnp.dot(ident_vars, var_table, preferred_element_type=jnp.float32)
    query_unit = unit_rows(agg_query.astype(jnp.float32))
    kv_mat = agg_kv.reshape(D, 2 * D)
    pos_rows = jnp.tile(pos_table, (BATCH, 1)).astype(jnp.float32)
    head_mat = head_weight.reshape(D, VARS * PIX)
    state = fields
    outputs = []
    for step in range(STEPS):
        lead_ids = lead_index + step
        lead_hot = (lead_ids[:, None] == jnp.arange(LEADS, dtype=jnp.int32)[None, :]).astype(jnp.bfloat16)
        lead_rows = jnp.repeat(jnp.dot(lead_hot, lead_table, preferred_element_type=jnp.float32), PATCHES, axis=0)
        flat = state.astype(jnp.bfloat16).reshape(VARS, PIX, rows_all)

        def per_channel(carry, element):
            numer, denom = carry
            field_one, weight_one, bias_one = element
            tokens = (jnp.dot(field_one.T, weight_one, preferred_element_type=jnp.float32) + bias_one[None, :]).astype(jnp.bfloat16)
            keyval = jnp.dot(tokens, kv_mat, preferred_element_type=jnp.float32).reshape(rows_all, 2, HEADS, CHANNEL_WIDTH)
            key_unit = unit_rows(keyval[:, 0])
            affinity_raw = lax.optimization_barrier(jnp.sum(key_unit * query_unit[None], axis=-1)) * agg_temp[None, :] / CHANNEL_WIDTH
            score_exponent = jnp.exp(affinity_raw)
            return ((numer + score_exponent[:, :, None] * keyval[:, 1], denom + score_exponent), None)
        start = (jnp.zeros((rows_all, HEADS, CHANNEL_WIDTH), jnp.float32), jnp.zeros((rows_all, HEADS), jnp.float32))
        (numer, denom), _ = lax.scan(per_channel, start, (flat, embed_weight, var_rows))
        pooled = (numer / denom[:, :, None]).reshape(rows_all, D).astype(jnp.bfloat16)
        resid = jnp.dot(pooled, agg_out, preferred_element_type=jnp.float32) + pos_rows + lead_rows
        for layer in range(LAYERS):
            normed = layer_norm(resid, norm_gain[layer, 0]).astype(jnp.bfloat16)
            mixed = jnp.dot(normed, qkv_weight[layer].reshape(D, HEADS * 3 * CHANNEL_WIDTH), preferred_element_type=jnp.float32)
            mixed = mixed.reshape(BATCH, PATCHES, HEADS, 3 * CHANNEL_WIDTH)
            queries = rounded_value(unit_rows(mixed[..., :CHANNEL_WIDTH]))
            keys = rounded_value(unit_rows(mixed[..., CHANNEL_WIDTH:2 * CHANNEL_WIDTH]))
            values = rounded_value(mixed[..., 2 * CHANNEL_WIDTH:])

            def per_head(element):
                probe_vector_by_branch, match_vector_by_branch, content_vector_by_branch, sharpness_by_branch = element
                affinity_raw = jnp.einsum('biz,bnz->bin', probe_vector_by_branch.astype(jnp.float32), match_vector_by_branch.astype(jnp.float32)) * (sharpness_by_branch / CHANNEL_WIDTH)
                score_exponent = jnp.exp(affinity_raw)
                denom_h = lax.optimization_barrier(jnp.sum(score_exponent, axis=-1))
                numerator_per_head = jnp.einsum('ros,rsw->row', rounded_value(score_exponent).astype(jnp.float32), content_vector_by_branch.astype(jnp.float32))
                return (numerator_per_head / denom_h[..., None]).astype(jnp.bfloat16)
            attended = lax.map(per_head, (jnp.moveaxis(queries, 2, 0), jnp.moveaxis(keys, 2, 0), jnp.moveaxis(values, 2, 0), attn_temp[layer]))
            attended = jnp.moveaxis(attended, 0, 2).reshape(rows_all, D)
            resid = resid + jnp.dot(attended, out_weight[layer].reshape(D, D), preferred_element_type=jnp.float32)
            normed = layer_norm(resid, norm_gain[layer, 1]).astype(jnp.bfloat16)
            hidden = jax.nn.gelu(jnp.dot(normed, up_weight[layer], preferred_element_type=jnp.float32), approximate=False).astype(jnp.bfloat16)
            resid = resid + jnp.dot(hidden, down_weight[layer], preferred_element_type=jnp.float32)
        final = layer_norm(resid, final_gain).astype(jnp.bfloat16)
        delta = jnp.dot(final, head_mat, preferred_element_type=jnp.float32).reshape(BATCH, PATCHES, VARS, PIX)
        state = state + jnp.transpose(delta, (2, 3, 0, 1))
        outputs.append(state)
    return jnp.stack(outputs)
```

```python
import jax
import jax.numpy as jnp
from jax import lax
from jax.experimental import pallas as pl
from jax.experimental.pallas import tpu as pltpu
from jax.sharding import PartitionSpec as P

STEPS = 2
LAYERS = 2
EPS_NORM = 1e-05
EPS_UNIT = 1e-06
F32 = jnp.float32
BF16 = jnp.bfloat16
MESH = pl.DeviceIdType.MESH

VAR_OFFS = ((2, 1), (1, 1), (3, 1), (2, 0), (0, 1), (1, 0), (3, 0))
SEQ_OFFS = ((2, 1), (1, 1), (3, 1), (0, 1), (2, 0), (1, 0), (3, 0))


def dot(a, b):
    return lax.dot_general(a, b, (((1,), (0,)), ((), ())), preferred_element_type=F32)


def dot_t(a, b):
    return lax.dot_general(a, b, (((1,), (1,)), ((), ())), preferred_element_type=F32)


def layer_norm(values, gain):
    centre = values - jnp.mean(values, axis=-1, keepdims=True)
    spread = jnp.mean(centre * centre, axis=-1, keepdims=True)
    return centre * lax.rsqrt(spread + EPS_NORM) * gain


def kernel(
    fields, ids, lead, emb, vart, aquery, kv_h, aout_h, atemp, pos_h, leadt, gains,
    qkv_h, temp, wo_h, up_h, dn_h, fgain, head_h,
    out,
    wq, wkv, wo, wu, wd, kvv, aout, headp, posv,
    fsnd, st, we, vr, vrt, mb, bb, kb, k2, vv, wb, nd, ndx, ndr, hexp, qexp,
    resid, xg, pb, rsb, qb, qx, kvb, kvo, ax, ab, fb, db, dlr,
    s_loc, s_ws, s_wr, s_is, s_ir, s_es, s_er, s_vs, s_vr, s_ag_s, s_ag_r, s_rs_s, s_rs_r,
    s_kv_s, s_kv_r, s_px_s, s_px_r, s_d_s, s_d_r,
):
    s = lax.axis_index("seq")
    v = lax.axis_index("var")
    i = v % 2
    p = v // 2
    px = p % 4
    py = p // 4
    sz = s // 2
    sy = s % 2
    other = (s, p * 2 + (1 - i))

    var_dst = []
    var_src = []
    for dx, dy in VAR_OFFS:
        var_dst.append(((py + dy) % 2) * 4 + (px + dx) % 4)
        var_src.append(((py + 2 - dy) % 2) * 4 + (px + 4 - dx) % 4)
    seq_dst = []
    seq_src = []
    for dz, dy in SEQ_OFFS:
        seq_dst.append(((sz + dz) % 4) * 2 + (sy + dy) % 2)
        seq_src.append(((sz + 4 - dz) % 4) * 2 + (sy + 2 - dy) % 2)

    def var_dev(q):
        return (s, q * 2 + i)

    def remote(src, dst, send, recv, dev):
        return pltpu.make_async_remote_copy(
            src_ref=src, dst_ref=dst, send_sem=send, recv_sem=recv, device_id=dev, device_id_type=MESH
        )

    own_heads = ((qkv_h.at[:, pl.ds(0, 64)], wq.at[i, :, pl.ds(0, 64)]),
                 (qkv_h.at[:, pl.ds(64, 128)], wkv.at[i]),
                 (wo_h, wo.at[i, :, pl.ds(64, 64)]),
                 (up_h, wu.at[i]),
                 (dn_h, wd.at[i]))
    loads = [pltpu.make_async_copy(kv_h, kvv, s_loc.at[0]),
             pltpu.make_async_copy(emb, we.at[p], s_loc.at[1]),
             pltpu.make_async_copy(aout_h, aout, s_loc.at[2]),
             pltpu.make_async_copy(pos_h.at[pl.ds(v * 16, 16)], posv, s_loc.at[3]),
             pltpu.make_async_copy(head_h.at[:, i], headp.at[:, pl.ds(0, 48)], s_loc.at[4])]
    for k, (a, b) in enumerate(own_heads):
        loads.append(pltpu.make_async_copy(a, b, s_loc.at[5 + k]))
    for c in loads:
        c.start()

    bar = pltpu.get_barrier_semaphore()
    for q in var_dst:
        pl.semaphore_signal(bar, inc=1, device_id=var_dev(q), device_id_type=MESH)
    for t in seq_dst:
        for j in range(2):
            pl.semaphore_signal(bar, inc=1, device_id=(t, p * 2 + j), device_id_type=MESH)
    pl.semaphore_signal(bar, inc=1, device_id=other, device_id_type=MESH)

    lane16 = lax.broadcasted_iota(jnp.int32, (32, 48), 1) // 16
    fpad = jnp.concatenate([fields[...], jnp.zeros((80, 256), F32)], axis=0)
    fsnd[...] = jnp.transpose(fpad).reshape(8, 32, 128)
    row8 = lax.broadcasted_iota(jnp.int32, (8, 48), 0)
    ch8 = lax.broadcasted_iota(jnp.int32, (8, 48), 1)
    named = jnp.where(row8 == 0, ids[0], jnp.where(row8 == 1, ids[1], ids[2]))
    hot = jnp.where((named == ch8) & (row8 < 3), 1.0, 0.0).astype(BF16)
    vrt[...] = dot(hot, vart[...]).astype(BF16)

    pl.semaphore_wait(bar, 22)

    init = []
    for k in range(7):
        init.append(remote(fsnd.at[var_dst[k]], st.at[p], s_is.at[k], s_ir.at[k], var_dev(var_dst[k])))
        init.append(remote(vrt, vr.at[p], s_vs.at[k], s_vr.at[k], var_dev(var_dst[k])))
        init.append(remote(emb, we.at[p], s_es.at[k], s_er.at[k], var_dev(var_dst[k])))
    for c in init:
        c.start()
    wcopies = []
    for k, (a, b) in enumerate(own_heads):
        wcopies.append(remote(a, b, s_ws.at[k], s_wr.at[k], other))
    for c in wcopies:
        c.start()

    st[p] = fsnd[p]
    vr[p] = vrt[...]
    wq[:, :, pl.ds(64, 64)] = jnp.zeros((2, LAYERS, 64, 1024), BF16)
    wo[:, :, pl.ds(0, 64)] = jnp.zeros((2, LAYERS, 64, 1024), BF16)
    headp[:, pl.ds(48, 80)] = jnp.zeros((8, 80, 1024), BF16)

    hrow = lax.broadcasted_iota(jnp.int32, (128, 1024), 0)
    hcol = lax.broadcasted_iota(jnp.int32, (128, 1024), 1) // 64
    hexp[...] = jnp.where(hrow == hcol, 1.0, 0.0).astype(BF16)
    aq = aquery[...].astype(F32)
    aq = aq * lax.rsqrt(jnp.mean(aq * aq, axis=-1, keepdims=True) + EPS_UNIT)
    aqt = jnp.concatenate([aq] * 16, axis=1)
    aqt = jnp.concatenate([aqt, jnp.zeros((112, 1024), F32)], axis=0)
    qexp[...] = jnp.where(hrow == hcol, aqt, 0.0).astype(BF16)
    tvec = jnp.concatenate([atemp[...] * (1.0 / 64.0), jnp.zeros((1, 112), F32)], axis=1)

    loads[0].wait()
    loads[1].wait()
    for k in range(7):
        remote(emb, we.at[var_src[k]], s_es.at[k], s_er.at[k], var_dev(var_dst[k])).wait_recv()
        remote(vrt, vr.at[var_src[k]], s_vs.at[k], s_vr.at[k], var_dev(var_dst[k])).wait_recv()

    wall = we[...].reshape(384, 1024)
    vall = vr[...].reshape(64, 1024)
    for n in range(4):
        cols = pl.ds(n * 512, 512)
        mb[:, :, cols] = dot(wall, kvv[:, cols]).astype(BF16).reshape(8, 48, 512)
        bb[:, :, cols] = dot(vall, kvv[:, cols]).reshape(8, 8, 512)
    for k in range(7):
        remote(fsnd.at[0], st.at[var_src[k]], s_is.at[k], s_ir.at[k], var_dev(var_dst[k])).wait_recv()
    for c in init:
        c.wait_send()
    for c in loads[2:5]:
        c.wait()

    lane128 = lax.broadcasted_iota(jnp.int32, (128, 128), 1)

    def partner(src, dst, k):
        return remote(src, dst, s_px_s.at[k], s_px_r.at[k], other)

    def gather_rows(normed, work):
        xg[p] = normed.astype(BF16)
        cs = [remote(xg.at[p], xg.at[p], s_ag_s.at[k], s_ag_r.at[k], var_dev(var_dst[k])) for k in range(7)]
        for c in cs:
            c.start()
        for k in range(7):
            remote(xg.at[p], xg.at[var_src[k]], s_ag_s.at[k], s_ag_r.at[k], var_dev(var_dst[k])).wait_recv()
        res = work(xg[...].reshape(128, 1024))
        for c in cs:
            c.wait_send()
        return res

    def sum_rows(part):
        pb[...] = part.astype(BF16).reshape(8, 16, 1024)
        cs = [remote(pb.at[var_dst[k]], rsb.at[k], s_rs_s.at[k], s_rs_r.at[k], var_dev(var_dst[k])) for k in range(7)]
        for c in cs:
            c.start()
        total = resid[...] + pb[p].astype(F32)
        for k in (6, 5, 4, 3, 2, 1, 0):
            cs[k].wait_recv()
            total = total + rsb[k].astype(F32)
        resid[...] = total
        for c in cs:
            c.wait_send()

    def step_body(step, carry):
        def pool_keys(q, c):
            sb = st[q][:, :48]
            blk = jnp.concatenate([jnp.where(lane16 == n, sb, 0.0) for n in range(3)], axis=0).astype(BF16)
            bias = bb[q]
            brow = jnp.concatenate([jnp.broadcast_to(bias[n:n + 1], (32, 2048)) for n in range(3)], axis=0)
            kk = dot(blk, mb[q, :, pl.ds(0, 1024)]) + brow[:, :1024]
            kb[q] = kk.astype(BF16)
            k2[q] = (kk * kk).astype(BF16)
            vv[q] = dot(blk, mb[q, :, pl.ds(1024, 1024)]) + brow[:, 1024:]
            return c

        lax.fori_loop(0, 8, pool_keys, 0)
        ss = dot_t(k2[...].reshape(768, 1024), hexp[...])
        qk = dot_t(kb[...].reshape(768, 1024), qexp[...])
        w = jnp.exp(qk * lax.rsqrt(ss * (1.0 / 64.0) + EPS_UNIT) * tvec)
        wb[...] = w.astype(BF16).reshape(8, 96, 128)
        nd[...] = jnp.zeros((32, 2048), F32)

        def pool_sum(q, c):
            wx = dot(wb[q], hexp[...])
            num = wx * vv[q]
            nd[:, pl.ds(0, 1024)] = nd[:, pl.ds(0, 1024)] + (num[0:32] + num[32:64] + num[64:96])
            nd[:, pl.ds(1024, 1024)] = nd[:, pl.ds(1024, 1024)] + (wx[0:32] + wx[32:64] + wx[64:96])
            return c

        lax.fori_loop(0, 8, pool_sum, 0)
        ndx[...] = nd[...].reshape(2, 16, 2048)
        c = partner(ndx.at[1 - i], ndr, 0)
        c.start()
        row16 = lax.broadcasted_iota(jnp.int32, (16, 16), 1)
        lhot = jnp.where(row16 == lead[0] + step, 1.0, 0.0).astype(BF16)
        add = posv[...].astype(F32) + dot(lhot, leadt[...])
        c.wait_recv()
        tot = ndx[i] + ndr[...]
        pooled = (tot[:, :1024] / tot[:, 1024:]).astype(BF16)
        c.wait_send()
        resid[...] = dot(pooled, aout[...]) + add

        @pl.when(step == 0)
        def _():
            for c in loads[5:]:
                c.wait()
            for c in wcopies:
                c.wait()

        def layer_body(l, carry):
            def qkv(x):
                kvs = []
                qs = []
                for h in range(2):
                    q = dot_t(x, wq[h, l])
                    q = q * lax.rsqrt(jnp.sum(q * q, axis=-1, keepdims=True) * (1.0 / 64.0) + EPS_UNIT)
                    qs.append(q.astype(BF16))
                    kv = dot_t(x, wkv[h, l])
                    kq = jnp.where(lane128 < 64, kv * kv, 0.0)
                    scale = lax.rsqrt(jnp.sum(kq, axis=-1, keepdims=True) * (1.0 / 64.0) + EPS_UNIT)
                    kvs.append((kv * jnp.where(lane128 < 64, scale, 1.0)).astype(BF16))
                return qs, kvs

            qs, kvs = gather_rows(layer_norm(resid[...], gains[l, pl.ds(0, 1), :]), qkv)
            kvo[0] = kvs[0]
            kvo[1] = kvs[1]
            cs = []
            for k in range(7):
                for j in range(2):
                    cs.append(remote(kvo.at[j], kvb.at[l, s, i], s_kv_s.at[2 * k + j],
                                     s_kv_r.at[l, 2 * k + i], (seq_dst[k], p * 2 + j)))
            for c in cs:
                c.start()
            qx[0] = qs[0]
            qx[1] = qs[1]
            cq = partner(qx.at[1 - i], qb.at[i], 1)
            cq.start()
            ck = partner(kvo.at[1 - i], kvb.at[l, s, i], 2)
            ck.start()
            qb[i] = qx[i]
            kvb[l, s, i] = kvo[i]
            partner(qx.at[1 - i], qb.at[1 - i], 1).wait_recv()
            partner(kvo.at[1 - i], kvb.at[l, s, 1 - i], 2).wait_recv()
            scale = temp[l, 0] * (1.0 / 64.0)
            q = qb[...].reshape(256, 128)
            num = jnp.zeros((256, 128), F32)
            den = jnp.zeros((256, 128), F32)
            for k in (7, 6, 5, 4, 3, 2, 1, 0):
                if k == 7:
                    src = s
                else:
                    src = seq_src[k]
                    for j in range(2):
                        remote(kvo.at[j], kvb.at[l, src, j], s_kv_s.at[2 * k + j],
                               s_kv_r.at[l, 2 * k + j], (seq_dst[k], p * 2 + j)).wait_recv()
                kv = kvb[l, src].reshape(256, 128)
                e = jnp.exp(dot_t(q, kv) * scale)
                den = den + e[:, :128] + e[:, 128:]
                num = num + dot(e.astype(BF16), kv)
            att = (num / jnp.sum(den, axis=-1, keepdims=True)).astype(BF16)
            ax[...] = att.reshape(2, 128, 128)
            ca = partner(ax.at[1 - i], ab, 3)
            ca.start()
            part = dot(ax[i], wo[i, l])
            ca.wait_recv()
            part = part + dot(ab[...], wo[1 - i, l])
            for c in cs:
                c.wait_send()
            cq.wait_send()
            ck.wait_send()
            ca.wait_send()
            sum_rows(part)

            def ffn(x):
                part = jnp.zeros((128, 1024), F32)
                for h in range(2):
                    hid = dot(x, wu[h, l])
                    hid = 0.5 * hid * (1.0 + lax.erf(hid * (0.5 ** 0.5)))
                    part = part + dot(hid.astype(BF16), wd[h, l])
                return part

            sum_rows(gather_rows(layer_norm(resid[...], gains[l, pl.ds(1, 1), :]), ffn))
            return carry

        lax.fori_loop(0, LAYERS, layer_body, 0)
        fb[i] = layer_norm(resid[...], fgain[...]).astype(BF16)
        c = partner(fb.at[i], fb.at[i], 4)
        c.start()
        partner(fb.at[i], fb.at[1 - i], 4).wait_recv()
        fin = fb[...].reshape(32, 1024)
        for q in range(8):
            d = dot_t(fin, headp[q])
            st[q] = st[q] + d
            db[step, q] = d.astype(BF16)
        c.wait_send()
        for k in range(7):
            remote(db.at[step, var_dst[k]], dlr.at[step, p], s_d_s.at[step, k], s_d_r.at[step, k],
                   var_dev(var_dst[k])).start()
        dlr[step, p] = db[step, p]
        return carry

    lax.fori_loop(0, STEPS, step_body, 0)

    state = fields[...]
    for step in range(STEPS):
        for k in range(7):
            c = remote(db.at[step, var_dst[k]], dlr.at[step, var_src[k]], s_d_s.at[step, k],
                       s_d_r.at[step, k], var_dev(var_dst[k]))
            c.wait_recv()
            c.wait_send()
        d = jnp.transpose(dlr[step].astype(F32).reshape(256, 128))
        state = state + d[:48]
        out[step] = state


def per_device(
    fields, channel_ids, lead_index, embed_weight, var_table, agg_query, agg_kv, agg_out,
    agg_temp, pos_table, lead_table, norm_gain, qkv_weight, attn_temp, out_weight,
    up_weight, down_weight, final_gain, head_weight,
):
    vm = pl.BlockSpec(memory_space=pltpu.VMEM)
    sm = pl.BlockSpec(memory_space=pltpu.SMEM)
    hb = pl.BlockSpec(memory_space=pl.ANY)
    dma = pltpu.SemaphoreType.DMA
    V = pltpu.VMEM
    qkv_t = jnp.transpose(qkv_weight, (0, 2, 3, 1)).reshape(LAYERS, 192, 1024)
    head_t = jnp.transpose(head_weight, (1, 2, 0)).reshape(8, 2, 48, 1024)
    out = pl.pallas_call(
        kernel,
        out_shape=jax.ShapeDtypeStruct((STEPS, 48, 256), F32),
        in_specs=[vm, sm, sm, hb, vm, vm, hb, hb, vm, hb, vm, vm, hb, sm, hb, hb, hb, vm, hb],
        out_specs=vm,
        scratch_shapes=[
            V((2, LAYERS, 128, 1024), BF16),
            V((2, LAYERS, 128, 1024), BF16),
            V((2, LAYERS, 128, 1024), BF16),
            V((2, LAYERS, 1024, 256), BF16),
            V((2, LAYERS, 256, 1024), BF16),
            V((1024, 2048), BF16),
            V((1024, 1024), BF16),
            V((8, 128, 1024), BF16),
            V((16, 1024), BF16),
            V((8, 32, 128), F32),
            V((8, 32, 128), F32),
            V((8, 48, 1024), BF16),
            V((8, 8, 1024), BF16),
            V((8, 1024), BF16),
            V((8, 48, 2048), BF16),
            V((8, 8, 2048), F32),
            V((8, 96, 1024), BF16),
            V((8, 96, 1024), BF16),
            V((8, 96, 1024), F32),
            V((8, 96, 128), BF16),
            V((32, 2048), F32),
            V((2, 16, 2048), F32),
            V((16, 2048), F32),
            V((128, 1024), BF16),
            V((128, 1024), BF16),
            V((16, 1024), F32),
            V((8, 16, 1024), BF16),
            V((8, 16, 1024), BF16),
            V((7, 16, 1024), BF16),
            V((2, 128, 128), BF16),
            V((2, 128, 128), BF16),
            V((LAYERS, 8, 2, 128, 128), BF16),
            V((2, 128, 128), BF16),
            V((2, 128, 128), BF16),
            V((128, 128), BF16),
            V((2, 16, 1024), BF16),
            V((STEPS, 8, 32, 128), BF16),
            V((STEPS, 8, 32, 128), BF16),
            dma((10,)),
            dma((5,)), dma((5,)),
            dma((7,)), dma((7,)),
            dma((7,)), dma((7,)),
            dma((7,)), dma((7,)),
            dma((7,)), dma((7,)),
            dma((7,)), dma((7,)),
            dma((14,)), dma((LAYERS, 14)),
            dma((5,)), dma((5,)),
            dma((STEPS, 7)), dma((STEPS, 7)),
        ],
        compiler_params=pltpu.CompilerParams(
            collective_id=0, has_side_effects=True, vmem_limit_bytes=60 * 1024 * 1024
        ),
        name="rollout",
    )(
        fields.reshape(48, 256),
        channel_ids,
        lead_index,
        embed_weight.reshape(48, 1024),
        var_table,
        agg_query,
        agg_kv.reshape(1024, 2048),
        agg_out,
        agg_temp.reshape(1, 16),
        pos_table,
        lead_table,
        norm_gain,
        qkv_t,
        attn_temp,
        out_weight.reshape(LAYERS, 64, 1024),
        up_weight,
        down_weight,
        final_gain.reshape(1, 1024),
        head_t,
    )
    return out.reshape(STEPS, 3, 16, 1, 256)


def solution(mesh):
    return jax.shard_map(
        per_device,
        mesh=mesh,
        in_specs=(
            P("var", None, None, "seq"),
            P("var"),
            P(),
            P("var", None, None),
            P(),
            P(),
            P(),
            P(),
            P(),
            P("seq", None),
            P(),
            P(),
            P(None, None, "var", None),
            P(None, "var"),
            P(None, "var", None, None),
            P(None, None, "var"),
            P(None, "var", None),
            P(),
            P(),
        ),
        out_specs=P(None, "var", None, None, "seq"),
        check_vma=False,
    )
```

```python
import jax
import jax.numpy as jnp
from jax import lax
from jax.experimental import pallas as pl
from jax.experimental.pallas import tpu as pltpu
from jax.sharding import PartitionSpec as P

STEPS = 2
LAYERS = 2
EPS_NORM = 1e-05
EPS_UNIT = 1e-06
F32 = jnp.float32
BF16 = jnp.bfloat16
MESH = pl.DeviceIdType.MESH

VAR_OFFS = ((2, 1), (1, 1), (3, 1), (2, 0), (0, 1), (1, 0), (3, 0))
SEQ_OFFS = ((2, 1), (1, 1), (3, 1), (0, 1), (2, 0), (1, 0), (3, 0))


def dot(a, b):
    return lax.dot_general(a, b, (((1,), (0,)), ((), ())), preferred_element_type=F32)


def dot_t(a, b):
    return lax.dot_general(a, b, (((1,), (1,)), ((), ())), preferred_element_type=F32)


def layer_norm(values, gain):
    centre = values - jnp.mean(values, axis=-1, keepdims=True)
    spread = jnp.mean(centre * centre, axis=-1, keepdims=True)
    return centre * lax.rsqrt(spread + EPS_NORM) * gain


def kernel(
    ids, lead, temp, fields_h, emb, vart_h, aquery_h, kv_h, aout_h, atemp_h, pos_h, leadt_h, gains_h,
    qkv_h, wo_h, up_h, dn_h, fgain_h, head_h,
    out,
    fields, vart, aquery, atemp, leadt, gains, fgain, kv3,
    wq, wkv, wo, wu, wd, kvv, aout, headp, posv,
    fsnd, st, we, mb, kb, k2, vv, wb, ndx, ndr, hexp, qexp,
    resid, xg, pb, rsb, qb, qx, kvb, kvo, ax, ab, fb, db, dlr,
    s_loc, s_ws, s_wr, s_is, s_ir, s_es, s_er, s_ag_s, s_ag_r, s_rs_s, s_rs_r,
    s_kv_s, s_kv_r, s_px_s, s_px_r, s_d_s, s_d_r,
):
    s = lax.axis_index("seq")
    v = lax.axis_index("var")
    i = v % 2
    p = v // 2
    px = p % 4
    py = p // 4
    sz = s // 2
    sy = s % 2
    other = (s, p * 2 + (1 - i))

    var_dst = []
    var_src = []
    for dx, dy in VAR_OFFS:
        var_dst.append(((py + dy) % 2) * 4 + (px + dx) % 4)
        var_src.append(((py + 2 - dy) % 2) * 4 + (px + 4 - dx) % 4)
    seq_dst = []
    seq_src = []
    for dz, dy in SEQ_OFFS:
        seq_dst.append(((sz + dz) % 4) * 2 + (sy + dy) % 2)
        seq_src.append(((sz + 4 - dz) % 4) * 2 + (sy + 2 - dy) % 2)

    def var_dev(q):
        return (s, q * 2 + i)

    def remote(src, dst, send, recv, dev):
        return pltpu.make_async_remote_copy(
            src_ref=src, dst_ref=dst, send_sem=send, recv_sem=recv, device_id=dev, device_id_type=MESH
        )

    own_heads = ((qkv_h.at[:, pl.ds(0, 64)], wq.at[i, :, pl.ds(0, 64)]),
                 (qkv_h.at[:, pl.ds(64, 128)], wkv.at[i]),
                 (wo_h, wo.at[i, :, pl.ds(64, 64)]),
                 (up_h, wu.at[i]),
                 (dn_h, wd.at[i]))
    loads = []
    for k, (a, b) in enumerate((
        (fields_h, fields), (kv_h, kv3), (emb, we.at[p]), (aquery_h, aquery), (vart_h, vart), (atemp_h, atemp),
        (aout_h, aout), (pos_h.at[pl.ds(v * 16, 16)], posv), (leadt_h, leadt), (gains_h, gains),
        (fgain_h, fgain), (head_h.at[:, i], headp.at[:, pl.ds(0, 48)]), *own_heads,
    )):
        loads.append(pltpu.make_async_copy(a, b, s_loc.at[k]))
    for c in loads[:6]:
        c.start()

    bar = pltpu.get_barrier_semaphore()
    for q in var_dst:
        pl.semaphore_signal(bar, inc=1, device_id=var_dev(q), device_id_type=MESH)
    for t in seq_dst:
        for j in range(2):
            pl.semaphore_signal(bar, inc=1, device_id=(t, p * 2 + j), device_id_type=MESH)
    pl.semaphore_signal(bar, inc=1, device_id=other, device_id_type=MESH)

    for c in loads[6:]:
        c.start()
    loads[0].wait()
    state0 = fields[:, 0, :]
    frow = lax.broadcasted_iota(jnp.int32, (80, 256), 0)
    fcol = lax.broadcasted_iota(jnp.int32, (80, 256), 1) % 32
    named = jnp.where(fcol == 0, ids[0], jnp.where(fcol == 1, ids[1], jnp.where(fcol == 2, ids[2], 0)))
    extra = jnp.where(frow == 0, named, 0).astype(F32)
    fsnd[...] = jnp.transpose(jnp.concatenate([state0, extra], axis=0)).reshape(8, 32, 128)

    pl.semaphore_wait(bar, 22)

    init = []
    for k in range(7):
        init.append(remote(fsnd.at[var_dst[k]], st.at[p], s_is.at[k], s_ir.at[k], var_dev(var_dst[k])))
        init.append(remote(emb, we.at[p], s_es.at[k], s_er.at[k], var_dev(var_dst[k])))
    for c in init:
        c.start()
    wcopies = []
    for k, (a, b) in enumerate(own_heads):
        wcopies.append(remote(a, b, s_ws.at[k], s_wr.at[k], other))
    for c in wcopies:
        c.start()

    st[p] = fsnd[p]
    wq[:, :, pl.ds(64, 64)] = jnp.zeros((2, LAYERS, 64, 1024), BF16)
    wo[:, :, pl.ds(0, 64)] = jnp.zeros((2, LAYERS, 64, 1024), BF16)
    headp[:, pl.ds(48, 80)] = jnp.zeros((8, 80, 1024), BF16)

    hrow = lax.broadcasted_iota(jnp.int32, (128, 1024), 0)
    hcol = lax.broadcasted_iota(jnp.int32, (128, 1024), 1) // 64
    hexp[...] = jnp.where(hrow == hcol, 1.0, 0.0).astype(BF16)
    loads[3].wait()
    aq = aquery[...].astype(F32)
    aq = aq * lax.rsqrt(jnp.mean(aq * aq, axis=-1, keepdims=True) + EPS_UNIT)
    aqt = jnp.concatenate([aq] * 16, axis=1)
    aqt = jnp.concatenate([aqt, jnp.zeros((112, 1024), F32)], axis=0)
    qexp[...] = jnp.where(hrow == hcol, aqt, 0.0).astype(BF16)
    for c in loads[4:6]:
        c.wait()
    tvec = jnp.concatenate([atemp[...] * (1.0 / 64.0), jnp.zeros((1, 112), F32)], axis=1)

    loads[1].wait()

    def split_kv(n, c):
        rows = pl.ds(n * 64, 64)
        kvv[rows] = kv3[rows].reshape(64, 2048)
        return c

    lax.fori_loop(0, 16, split_kv, 0)
    loads[2].wait()
    for k in range(7):
        remote(fsnd.at[0], st.at[var_src[k]], s_is.at[k], s_ir.at[k], var_dev(var_dst[k])).wait_recv()
    nrow = lax.broadcasted_iota(jnp.int32, (128, 48), 0) % 16
    ncol = lax.broadcasted_iota(jnp.int32, (128, 48), 1).astype(F32)
    named = st[:, pl.ds(0, 16)].reshape(128, 128)[:, 48:49]
    hot = jnp.where((named == ncol) & (nrow < 3), 1.0, 0.0).astype(BF16)
    vall = dot(hot, vart[...]).astype(BF16)
    for n in range(4):
        cols = pl.ds(n * 512, 512)
        mb[:, pl.ds(48, 16), cols] = dot(vall, kvv[:, cols]).astype(BF16).reshape(8, 16, 512)
    for k in range(7):
        remote(emb, we.at[var_src[k]], s_es.at[k], s_er.at[k], var_dev(var_dst[k])).wait_recv()
    wall = we[...].reshape(384, 1024)
    for n in range(4):
        cols = pl.ds(n * 512, 512)
        mb[:, pl.ds(0, 48), cols] = dot(wall, kvv[:, cols]).astype(BF16).reshape(8, 48, 512)
    for c in init:
        c.wait_send()
    for c in loads[6:12]:
        c.wait()

    lane64 = lax.broadcasted_iota(jnp.int32, (32, 64), 1)
    lane128 = lax.broadcasted_iota(jnp.int32, (128, 128), 1)

    def partner(src, dst, k):
        return remote(src, dst, s_px_s.at[k], s_px_r.at[k], other)

    def gather_rows(normed):
        xg[p] = normed.astype(BF16)
        cs = [remote(xg.at[p], xg.at[p], s_ag_s.at[k], s_ag_r.at[k], var_dev(var_dst[k])) for k in range(7)]
        for c in cs:
            c.start()
        for k in range(7):
            remote(xg.at[p], xg.at[var_src[k]], s_ag_s.at[k], s_ag_r.at[k], var_dev(var_dst[k])).wait_recv()
        return xg[...].reshape(128, 1024), cs

    def sum_rows(part):
        pb[...] = part.astype(BF16).reshape(8, 16, 1024)
        cs = [remote(pb.at[var_dst[k]], rsb.at[k], s_rs_s.at[k], s_rs_r.at[k], var_dev(var_dst[k])) for k in range(7)]
        for c in cs:
            c.start()
        total = resid[...] + pb[p].astype(F32)
        for k in (6, 5, 4, 3, 2, 1, 0):
            cs[k].wait_recv()
            total = total + rsb[k].astype(F32)
        resid[...] = total
        for c in cs:
            c.wait_send()

    def step_body(step, carry):
        for q in range(8):
            sb = st[q][:, :64]
            blk = jnp.concatenate(
                [jnp.where(lane64 // 16 == n, sb, jnp.where(lane64 == 48 + n, 1.0, 0.0)) for n in range(3)], axis=0
            ).astype(BF16)
            kk = dot(blk, mb[q, :, pl.ds(0, 1024)])
            kb[q] = kk.astype(BF16)
            k2[q] = (kk * kk).astype(BF16)
            vv[q] = dot(blk, mb[q, :, pl.ds(1024, 1024)]).astype(BF16)
        ss = dot_t(k2[...].reshape(768, 1024), hexp[...])
        qk = dot_t(kb[...].reshape(768, 1024), qexp[...])
        w = jnp.exp(qk * lax.rsqrt(ss * (1.0 / 64.0) + EPS_UNIT) * tvec)
        wb[...] = w.astype(BF16).reshape(8, 96, 128)
        num = jnp.zeros((32, 1024), F32)
        den = jnp.zeros((32, 1024), F32)
        for q in range(8):
            wx = dot(wb[q], hexp[...])
            nx = wx * vv[q].astype(F32)
            num = num + (nx[0:32] + nx[32:64] + nx[64:96])
            den = den + (wx[0:32] + wx[32:64] + wx[64:96])
        ndx[:, :, pl.ds(0, 1024)] = num.reshape(2, 16, 1024)
        ndx[:, :, pl.ds(1024, 1024)] = den.reshape(2, 16, 1024)
        c = partner(ndx.at[1 - i], ndr, 0)
        c.start()
        row16 = lax.broadcasted_iota(jnp.int32, (16, 16), 1)
        lhot = jnp.where(row16 == lead[0] + step, 1.0, 0.0).astype(BF16)
        add = posv[...].astype(F32) + dot(lhot, leadt[...])
        c.wait_recv()
        tot = ndx[i] + ndr[...]
        pooled = (tot[:, :1024] / tot[:, 1024:]).astype(BF16)
        c.wait_send()
        resid[...] = dot(pooled, aout[...]) + add

        @pl.when(step == 0)
        def _():
            for c in loads[12:]:
                c.wait()
            for c in wcopies:
                c.wait()

        def layer_body(l, carry):
            x, cg = gather_rows(layer_norm(resid[...], gains[l, pl.ds(0, 1), :]))
            cs = []
            for h in range(2):
                kv = dot_t(x, wkv[h, l])
                kq = jnp.where(lane128 < 64, kv * kv, 0.0)
                scale = lax.rsqrt(jnp.sum(kq, axis=-1, keepdims=True) * (1.0 / 64.0) + EPS_UNIT)
                kvo[h] = (kv * jnp.where(lane128 < 64, scale, 1.0)).astype(BF16)
                for k in range(7):
                    c = remote(kvo.at[h], kvb.at[l, s, i], s_kv_s.at[2 * k + h],
                               s_kv_r.at[l, 2 * k + i], (seq_dst[k], p * 2 + h))
                    c.start()
                    cs.append(c)
            ck = partner(kvo.at[1 - i], kvb.at[l, s, i], 2)
            ck.start()
            for h in range(2):
                q = dot_t(x, wq[h, l])
                q = q * lax.rsqrt(jnp.sum(q * q, axis=-1, keepdims=True) * (1.0 / 64.0) + EPS_UNIT)
                qx[h] = q.astype(BF16)
            cq = partner(qx.at[1 - i], qb.at[i], 1)
            cq.start()
            qb[i] = qx[i]
            kvb[l, s, i] = kvo[i]
            for c in cg:
                c.wait_send()
            partner(qx.at[1 - i], qb.at[1 - i], 1).wait_recv()
            partner(kvo.at[1 - i], kvb.at[l, s, 1 - i], 2).wait_recv()
            scale = temp[l] * (1.0 / 64.0)
            q = qb[...].reshape(256, 128)
            num = jnp.zeros((256, 128), F32)
            den = jnp.zeros((256, 128), F32)
            for k in (7, 6, 5, 4, 3, 2, 1, 0):
                if k == 7:
                    src = s
                else:
                    src = seq_src[k]
                    for j in range(2):
                        remote(kvo.at[j], kvb.at[l, src, j], s_kv_s.at[2 * k + j],
                               s_kv_r.at[l, 2 * k + j], (seq_dst[k], p * 2 + j)).wait_recv()
                kv = kvb[l, src].reshape(256, 128)
                e = jnp.exp(dot_t(q, kv) * scale)
                den = den + e[:, :128] + e[:, 128:]
                num = num + dot(e.astype(BF16), kv)
            att = (num / jnp.sum(den, axis=-1, keepdims=True)).astype(BF16)
            ax[...] = att.reshape(2, 128, 128)
            ca = partner(ax.at[1 - i], ab, 3)
            ca.start()
            part = dot(ax[i], wo[i, l])
            ca.wait_recv()
            part = part + dot(ab[...], wo[1 - i, l])
            for c in cs:
                c.wait_send()
            cq.wait_send()
            ck.wait_send()
            ca.wait_send()
            sum_rows(part)

            x, cg = gather_rows(layer_norm(resid[...], gains[l, pl.ds(1, 1), :]))
            part = jnp.zeros((128, 1024), F32)
            for h in range(2):
                hid = dot(x, wu[h, l])
                hid = 0.5 * hid * (1.0 + lax.erf(hid * (0.5 ** 0.5)))
                part = part + dot(hid.astype(BF16), wd[h, l])
            for c in cg:
                c.wait_send()
            sum_rows(part)
            return carry

        lax.fori_loop(0, LAYERS, layer_body, 0)
        fb[i] = layer_norm(resid[...], fgain[...]).astype(BF16)
        c = partner(fb.at[i], fb.at[i], 4)
        c.start()
        partner(fb.at[i], fb.at[1 - i], 4).wait_recv()
        fin = fb[...].reshape(32, 1024)
        for q in range(8):
            d = dot_t(fin, headp[q])
            st[q] = st[q] + d
            db[step, q] = d.astype(BF16)
        c.wait_send()
        for k in range(7):
            remote(db.at[step, var_dst[k]], dlr.at[step, p], s_d_s.at[step, k], s_d_r.at[step, k],
                   var_dev(var_dst[k])).start()
        dlr[step, p] = db[step, p]
        return carry

    lax.fori_loop(0, STEPS, step_body, 0)

    state = fields[:, 0, :]
    for step in range(STEPS):
        for k in range(7):
            c = remote(db.at[step, var_dst[k]], dlr.at[step, var_src[k]], s_d_s.at[step, k],
                       s_d_r.at[step, k], var_dev(var_dst[k]))
            c.wait_recv()
            c.wait_send()
        d = jnp.transpose(dlr[step].astype(F32).reshape(256, 128))
        state = state + d[:48]
        out[step] = state.reshape(48, 1, 256)


def per_device(
    fields, channel_ids, lead_index, embed_weight, var_table, agg_query, agg_kv, agg_out,
    agg_temp, pos_table, lead_table, norm_gain, qkv_weight, attn_temp, out_weight,
    up_weight, down_weight, final_gain, head_weight,
):
    vm = pl.BlockSpec(memory_space=pltpu.VMEM)
    sm = pl.BlockSpec(memory_space=pltpu.SMEM)
    hb = pl.BlockSpec(memory_space=pl.ANY)
    dma = pltpu.SemaphoreType.DMA
    V = pltpu.VMEM
    qkv_t = jnp.transpose(qkv_weight, (0, 2, 3, 1)).reshape(LAYERS, 192, 1024)
    head_t = jnp.transpose(head_weight, (1, 2, 0)).reshape(8, 2, 48, 1024)
    out = pl.pallas_call(
        kernel,
        out_shape=jax.ShapeDtypeStruct((STEPS, 48, 1, 256), F32),
        in_specs=[sm] * 3 + [hb] * 16,
        out_specs=vm,
        scratch_shapes=[
            V((48, 1, 256), F32),
            V((48, 1024), BF16),
            V((16, 64), BF16),
            V((1, 16), F32),
            V((16, 1024), BF16),
            V((LAYERS, 2, 1024), F32),
            V((1, 1024), F32),
            V((1024, 2, 1024), BF16),
            V((2, LAYERS, 128, 1024), BF16),
            V((2, LAYERS, 128, 1024), BF16),
            V((2, LAYERS, 128, 1024), BF16),
            V((2, LAYERS, 1024, 256), BF16),
            V((2, LAYERS, 256, 1024), BF16),
            V((1024, 2048), BF16),
            V((1024, 1024), BF16),
            V((8, 128, 1024), BF16),
            V((16, 1024), BF16),
            V((8, 32, 128), F32),
            V((8, 32, 128), F32),
            V((8, 48, 1024), BF16),
            V((8, 64, 2048), BF16),
            V((8, 96, 1024), BF16),
            V((8, 96, 1024), BF16),
            V((8, 96, 1024), BF16),
            V((8, 96, 128), BF16),
            V((2, 16, 2048), F32),
            V((16, 2048), F32),
            V((128, 1024), BF16),
            V((128, 1024), BF16),
            V((16, 1024), F32),
            V((8, 16, 1024), BF16),
            V((8, 16, 1024), BF16),
            V((7, 16, 1024), BF16),
            V((2, 128, 128), BF16),
            V((2, 128, 128), BF16),
            V((LAYERS, 8, 2, 128, 128), BF16),
            V((2, 128, 128), BF16),
            V((2, 128, 128), BF16),
            V((128, 128), BF16),
            V((2, 16, 1024), BF16),
            V((STEPS, 8, 32, 128), BF16),
            V((STEPS, 8, 32, 128), BF16),
            dma((17,)),
            dma((5,)), dma((5,)),
            dma((7,)), dma((7,)),
            dma((7,)), dma((7,)),
            dma((7,)), dma((7,)),
            dma((7,)), dma((7,)),
            dma((14,)), dma((LAYERS, 14)),
            dma((5,)), dma((5,)),
            dma((STEPS, 7)), dma((STEPS, 7)),
        ],
        compiler_params=pltpu.CompilerParams(
            collective_id=0, has_side_effects=True, vmem_limit_bytes=60 * 1024 * 1024
        ),
        name="rollout",
    )(
        channel_ids,
        lead_index,
        attn_temp.reshape(LAYERS),
        fields.reshape(48, 1, 256),
        embed_weight.reshape(48, 1024),
        var_table,
        agg_query,
        agg_kv,
        agg_out,
        agg_temp.reshape(1, 16),
        pos_table,
        lead_table,
        norm_gain,
        qkv_t,
        out_weight.reshape(LAYERS, 64, 1024),
        up_weight,
        down_weight,
        final_gain.reshape(1, 1024),
        head_t,
    )
    return out.reshape(STEPS, 3, 16, 1, 256)


def solution(mesh):
    return jax.shard_map(
        per_device,
        mesh=mesh,
        in_specs=(
            P("var", None, None, "seq"),
            P("var"),
            P(),
            P("var", None, None),
            P(),
            P(),
            P(),
            P(),
            P(),
            P("seq", None),
            P(),
            P(),
            P(None, None, "var", None),
            P(None, "var"),
            P(None, "var", None, None),
            P(None, None, "var"),
            P(None, "var", None),
            P(),
            P(),
        ),
        out_specs=P(None, "var", None, None, "seq"),
        check_vma=False,
    )
```

```python
import jax
import jax.numpy as jnp
from jax import lax
from jax.experimental import pallas as pl
from jax.experimental.pallas import tpu as pltpu
from jax.sharding import PartitionSpec as P

STEPS = 2
LAYERS = 2
EPS_NORM = 1e-05
EPS_UNIT = 1e-06
F32 = jnp.float32
BF16 = jnp.bfloat16
MESH = pl.DeviceIdType.MESH

VAR_OFFS = ((2, 1), (1, 1), (3, 1), (2, 0), (0, 1), (1, 0), (3, 0))
SEQ_OFFS = ((2, 1), (1, 1), (3, 1), (0, 1), (2, 0), (1, 0), (3, 0))


def dot(a, b):
    return lax.dot_general(a, b, (((1,), (0,)), ((), ())), preferred_element_type=F32)


def dot_t(a, b):
    return lax.dot_general(a, b, (((1,), (1,)), ((), ())), preferred_element_type=F32)


def layer_norm(values, gain):
    centre = values - jnp.mean(values, axis=-1, keepdims=True)
    spread = jnp.mean(centre * centre, axis=-1, keepdims=True)
    return centre * lax.rsqrt(spread + EPS_NORM) * gain


def kernel(
    ids, lead, temp, fields_h, emb, vart_h, aquery_h, kv_h, aout_h, atemp_h, pos_h, leadt_h, gains_h,
    qkv_h, wo_h, up_h, dn_h, fgain_h, head_h,
    out,
    fields, vart, aquery, atemp, leadt, gains, fgain, kv3,
    wq, wkv, wo, wu, wd, kvv, aout, headp, posv,
    fsnd, st, we, mb, kb, k2, vv, wb, ndx, ndr, hexp, qexp,
    resid, xg, pb, rsb, qb, qx, kvb, kvo, ax, ab, at, rs, fb, db, dlr,
    s_loc, s_ws, s_wr, s_is, s_ir, s_es, s_er, s_ag_s, s_ag_r, s_rs_s, s_rs_r,
    s_kv_s, s_kv_r, s_px_s, s_px_r, s_d_s, s_d_r,
    s_at_s, s_at_r, s_wo_s, s_wo_r, s_wp_s, s_wp_r,
):
    s = lax.axis_index("seq")
    v = lax.axis_index("var")
    i = v % 2
    p = v // 2
    px = p % 4
    py = p // 4
    sz = s // 2
    sy = s % 2
    other = (s, p * 2 + (1 - i))

    var_dst = []
    var_src = []
    for dx, dy in VAR_OFFS:
        var_dst.append(((py + dy) % 2) * 4 + (px + dx) % 4)
        var_src.append(((py + 2 - dy) % 2) * 4 + (px + 4 - dx) % 4)
    seq_dst = []
    seq_src = []
    for dz, dy in SEQ_OFFS:
        seq_dst.append(((sz + dz) % 4) * 2 + (sy + dy) % 2)
        seq_src.append(((sz + 4 - dz) % 4) * 2 + (sy + 2 - dy) % 2)

    def var_dev(q):
        return (s, q * 2 + i)

    def remote(src, dst, send, recv, dev):
        return pltpu.make_async_remote_copy(
            src_ref=src, dst_ref=dst, send_sem=send, recv_sem=recv, device_id=dev, device_id_type=MESH
        )

    own_heads = ((qkv_h.at[:, pl.ds(0, 64)], wq.at[i, :, pl.ds(0, 64)]),
                 (qkv_h.at[:, pl.ds(64, 128)], wkv.at[i]),
                 (up_h, wu.at[i]),
                 (dn_h, wd.at[i]))
    loads = []
    for k, (a, b) in enumerate((
        (fields_h, fields), (kv_h, kv3), (emb, we.at[p]), (aquery_h, aquery), (vart_h, vart), (atemp_h, atemp),
        (aout_h, aout), (pos_h.at[pl.ds(v * 16, 16)], posv), (leadt_h, leadt), (gains_h, gains),
        (fgain_h, fgain), (head_h.at[:, i], headp.at[:, pl.ds(0, 48)]), *own_heads, (wo_h, wo.at[:, v]),
    )):
        loads.append(pltpu.make_async_copy(a, b, s_loc.at[k]))
    for c in loads[:6]:
        c.start()

    bar = pltpu.get_barrier_semaphore()
    for q in var_dst:
        for j in range(2):
            pl.semaphore_signal(bar, inc=1, device_id=(s, q * 2 + j), device_id_type=MESH)
    for t in seq_dst:
        for j in range(2):
            pl.semaphore_signal(bar, inc=1, device_id=(t, p * 2 + j), device_id_type=MESH)
    pl.semaphore_signal(bar, inc=1, device_id=other, device_id_type=MESH)

    for c in loads[6:]:
        c.start()
    loads[0].wait()
    state0 = fields[:, 0, :]
    frow = lax.broadcasted_iota(jnp.int32, (80, 256), 0)
    fcol = lax.broadcasted_iota(jnp.int32, (80, 256), 1) % 32
    named = jnp.where(fcol == 0, ids[0], jnp.where(fcol == 1, ids[1], jnp.where(fcol == 2, ids[2], 0)))
    extra = jnp.where(frow == 0, named, 0).astype(F32)
    fsnd[...] = jnp.transpose(jnp.concatenate([state0, extra], axis=0)).reshape(8, 32, 128)

    pl.semaphore_wait(bar, 29)

    init = []
    for k in range(7):
        init.append(remote(fsnd.at[var_dst[k]], st.at[p], s_is.at[k], s_ir.at[k], var_dev(var_dst[k])))
        init.append(remote(emb, we.at[p], s_es.at[k], s_er.at[k], var_dev(var_dst[k])))
    for c in init:
        c.start()
    wcopies = []
    for k, (a, b) in enumerate((*own_heads, (wo_h, wo.at[:, v]))):
        wcopies.append(remote(a, b, s_ws.at[k], s_wr.at[k], other))
    for c in wcopies:
        c.start()

    def wo_copy(l, k):
        return remote(wo_h.at[l], wo.at[l, v], s_wo_s.at[l, k], s_wo_r.at[l, k], var_dev(var_dst[k]))

    def wo_arrival(l, k):
        h = var_src[k] * 2 + i
        return remote(wo_h.at[l], wo.at[l, h], s_wo_s.at[l, k], s_wo_r.at[l, k], var_dev(var_dst[k]))

    def wo_pass(l, k):
        h = var_src[k] * 2 + i
        return remote(wo.at[l, h], wo.at[l, h], s_wp_s.at[l, k], s_wp_r.at[l, k], other)

    def wo_passed(l, k):
        h = var_src[k] * 2 + 1 - i
        return remote(wo.at[l, h], wo.at[l, h], s_wp_s.at[l, k], s_wp_r.at[l, k], other)

    for k in range(7):
        wo_copy(0, k).start()

    st[p] = fsnd[p]
    wq[:, :, pl.ds(64, 64)] = jnp.zeros((2, LAYERS, 64, 1024), BF16)
    headp[:, pl.ds(48, 80)] = jnp.zeros((8, 80, 1024), BF16)

    hrow = lax.broadcasted_iota(jnp.int32, (128, 1024), 0)
    hcol = lax.broadcasted_iota(jnp.int32, (128, 1024), 1) // 64
    hexp[...] = jnp.where(hrow == hcol, 1.0, 0.0).astype(BF16)
    loads[3].wait()
    aq = aquery[...].astype(F32)
    aq = aq * lax.rsqrt(jnp.mean(aq * aq, axis=-1, keepdims=True) + EPS_UNIT)
    aqt = jnp.concatenate([aq] * 16, axis=1)
    aqt = jnp.concatenate([aqt, jnp.zeros((112, 1024), F32)], axis=0)
    qexp[...] = jnp.where(hrow == hcol, aqt, 0.0).astype(BF16)
    for c in loads[4:6]:
        c.wait()
    tvec = jnp.concatenate([atemp[...] * (1.0 / 64.0), jnp.zeros((1, 112), F32)], axis=1)

    loads[1].wait()

    def split_kv(n, c):
        rows = pl.ds(n * 64, 64)
        kvv[rows] = kv3[rows].reshape(64, 2048)
        return c

    lax.fori_loop(0, 16, split_kv, 0)
    loads[2].wait()
    for k in range(7):
        remote(fsnd.at[0], st.at[var_src[k]], s_is.at[k], s_ir.at[k], var_dev(var_dst[k])).wait_recv()
    nrow = lax.broadcasted_iota(jnp.int32, (128, 48), 0) % 16
    ncol = lax.broadcasted_iota(jnp.int32, (128, 48), 1).astype(F32)
    named = st[:, pl.ds(0, 16)].reshape(128, 128)[:, 48:49]
    hot = jnp.where((named == ncol) & (nrow < 3), 1.0, 0.0).astype(BF16)
    vall = dot(hot, vart[...]).astype(BF16)
    for n in range(4):
        cols = pl.ds(n * 512, 512)
        mb[:, pl.ds(48, 16), cols] = dot(vall, kvv[:, cols]).astype(BF16).reshape(8, 16, 512)
    for k in range(7):
        remote(emb, we.at[var_src[k]], s_es.at[k], s_er.at[k], var_dev(var_dst[k])).wait_recv()
    wall = we[...].reshape(384, 1024)
    for n in range(4):
        cols = pl.ds(n * 512, 512)
        mb[:, pl.ds(0, 48), cols] = dot(wall, kvv[:, cols]).astype(BF16).reshape(8, 48, 512)
    for c in init:
        c.wait_send()
    for c in loads[6:12]:
        c.wait()

    lane64 = lax.broadcasted_iota(jnp.int32, (32, 64), 1)
    lane128 = lax.broadcasted_iota(jnp.int32, (128, 128), 1)

    def partner(src, dst, k):
        return remote(src, dst, s_px_s.at[k], s_px_r.at[k], other)

    def gather_rows(own):
        xg[p] = own.astype(BF16)
        cs = [remote(xg.at[p], xg.at[p], s_ag_s.at[k], s_ag_r.at[k], var_dev(var_dst[k])) for k in range(7)]
        for c in cs:
            c.start()
        for k in range(7):
            remote(xg.at[p], xg.at[var_src[k]], s_ag_s.at[k], s_ag_r.at[k], var_dev(var_dst[k])).wait_recv()
        return xg[...].reshape(128, 1024), cs

    def sum_rows(part):
        pb[...] = part.astype(BF16).reshape(8, 16, 1024)
        cs = [remote(pb.at[var_dst[k]], rsb.at[k], s_rs_s.at[k], s_rs_r.at[k], var_dev(var_dst[k])) for k in range(7)]
        for c in cs:
            c.start()
        total = rs[p] + pb[p].astype(F32)
        for k in (6, 5, 4, 3, 2, 1, 0):
            cs[k].wait_recv()
            total = total + rsb[k].astype(F32)
        resid[...] = total
        for c in cs:
            c.wait_send()

    def step_body(step, carry):
        for q in range(8):
            sb = st[q][:, :64]
            blk = jnp.concatenate(
                [jnp.where(lane64 // 16 == n, sb, jnp.where(lane64 == 48 + n, 1.0, 0.0)) for n in range(3)], axis=0
            ).astype(BF16)
            kk = dot(blk, mb[q, :, pl.ds(0, 1024)])
            kb[q] = kk.astype(BF16)
            k2[q] = (kk * kk).astype(BF16)
            vv[q] = dot(blk, mb[q, :, pl.ds(1024, 1024)]).astype(BF16)
        ss = dot_t(k2[...].reshape(768, 1024), hexp[...])
        qk = dot_t(kb[...].reshape(768, 1024), qexp[...])
        w = jnp.exp(qk * lax.rsqrt(ss * (1.0 / 64.0) + EPS_UNIT) * tvec)
        wb[...] = w.astype(BF16).reshape(8, 96, 128)
        num = jnp.zeros((32, 1024), F32)
        den = jnp.zeros((32, 1024), F32)
        for q in range(8):
            wx = dot(wb[q], hexp[...])
            nx = wx * vv[q].astype(F32)
            num = num + (nx[0:32] + nx[32:64] + nx[64:96])
            den = den + (wx[0:32] + wx[32:64] + wx[64:96])
        ndx[:, :, pl.ds(0, 1024)] = num.reshape(2, 16, 1024)
        ndx[:, :, pl.ds(1024, 1024)] = den.reshape(2, 16, 1024)
        c = partner(ndx.at[1 - i], ndr, 0)
        c.start()
        row16 = lax.broadcasted_iota(jnp.int32, (16, 16), 1)
        lhot = jnp.where(row16 == lead[0] + step, 1.0, 0.0).astype(BF16)
        add = posv[...].astype(F32) + dot(lhot, leadt[...])
        c.wait_recv()
        tot = ndx[i] + ndr[...]
        pooled = (tot[:, :1024] / tot[:, 1024:]).astype(BF16)
        c.wait_send()
        resid[...] = dot(pooled, aout[...]) + add

        @pl.when(step == 0)
        def _():
            for c in loads[12:]:
                c.wait()
            for c in wcopies[:4]:
                c.wait()
            wcopies[4].wait_send()
            remote(wo_h, wo.at[:, p * 2 + 1 - i], s_ws.at[4], s_wr.at[4], other).wait_recv()

        def layer_body(l, carry):
            x, cg = gather_rows(resid[...])

            rows = x.astype(F32)
            x = layer_norm(rows, gains[l, pl.ds(0, 1), :]).astype(BF16)
            cs = []
            for h in range(2):
                kv = dot_t(x, wkv[h, l])
                kq = jnp.where(lane128 < 64, kv * kv, 0.0)
                scale = lax.rsqrt(jnp.sum(kq, axis=-1, keepdims=True) * (1.0 / 64.0) + EPS_UNIT)
                kvo[h] = (kv * jnp.where(lane128 < 64, scale, 1.0)).astype(BF16)
                for k in range(7):
                    c = remote(kvo.at[h], kvb.at[l, s, i], s_kv_s.at[2 * k + h],
                               s_kv_r.at[l, 2 * k + i], (seq_dst[k], p * 2 + h))
                    c.start()
                    cs.append(c)
            ck = partner(kvo.at[1 - i], kvb.at[l, s, i], 2)
            ck.start()

            @pl.when((step == 0) & (l == 0))
            def _():
                for k in range(7):
                    wo_copy(1, k).start()

            for h in range(2):
                q = dot_t(x, wq[h, l])
                q = q * lax.rsqrt(jnp.sum(q * q, axis=-1, keepdims=True) * (1.0 / 64.0) + EPS_UNIT)
                qx[h] = q.astype(BF16)
            cq = partner(qx.at[1 - i], qb.at[i], 1)
            cq.start()
            qb[i] = qx[i]
            kvb[l, s, i] = kvo[i]

            @pl.when(step == 0)
            def _():
                for k in range(7):
                    wo_arrival(l, k).wait_recv()
                    wo_pass(l, k).start()

            for c in cg:
                c.wait_send()
            partner(qx.at[1 - i], qb.at[1 - i], 1).wait_recv()
            partner(kvo.at[1 - i], kvb.at[l, s, 1 - i], 2).wait_recv()
            scale = temp[l] * (1.0 / 64.0)
            q = qb[...].reshape(256, 128)
            num = jnp.zeros((256, 128), F32)
            den = jnp.zeros((256, 128), F32)
            for k in (7, 6, 5, 4, 3, 2, 1, 0):
                if k == 7:
                    src = s
                else:
                    src = seq_src[k]
                    for j in range(2):
                        remote(kvo.at[j], kvb.at[l, src, j], s_kv_s.at[2 * k + j],
                               s_kv_r.at[l, 2 * k + j], (seq_dst[k], p * 2 + j)).wait_recv()
                kv = kvb[l, src].reshape(256, 128)
                e = jnp.exp(dot_t(q, kv) * scale)
                den = den + e[:, :128] + e[:, 128:]
                num = num + dot(e.astype(BF16), kv)
            att = num / jnp.sum(den, axis=-1, keepdims=True)
            for h in range(2):
                lo, hi = att[128 * h : 128 * h + 64], att[128 * h + 64 : 128 * h + 128]
                ax[h] = jnp.where(lane128[:64] < 64, pltpu.roll(lo, 64, 1), hi).astype(BF16)
            ca = []
            for k in range(7):
                for j in range(2):
                    ca.append(remote(ax.at[j], ab.at[v], s_at_s.at[2 * k + j], s_at_r.at[2 * k + i],
                                     (s, var_dst[k] * 2 + j)))
            for c in ca:
                c.start()
            cp = partner(ax.at[1 - i], ab.at[v], 3)
            cp.start()
            ab[v] = ax[i]
            for c in cs:
                c.wait_send()
            cq.wait_send()
            ck.wait_send()

            @pl.when(step == 0)
            def _():
                for k in range(7):
                    wo_passed(l, k).wait_recv()
                    wo_pass(l, k).wait_send()
                    wo_copy(l, k).wait_send()

            partner(ax.at[1 - i], ab.at[p * 2 + 1 - i], 3).wait_recv()
            for k in range(7):
                for j in range(2):
                    remote(ax.at[j], ab.at[var_src[k] * 2 + j], s_at_s.at[2 * k + j], s_at_r.at[2 * k + j],
                           (s, var_dst[k] * 2 + j)).wait_recv()
            for q in range(8):
                even, odd = ab[2 * q].astype(F32), ab[2 * q + 1].astype(F32)
                cols = pl.ds(q * 128, 128)
                left = lane128[:64] < 64
                at[pl.ds(0, 64), cols] = jnp.where(left, even, pltpu.roll(odd, 64, 1)).astype(BF16)
                at[pl.ds(64, 64), cols] = jnp.where(left, pltpu.roll(even, 64, 1), odd).astype(BF16)
            rows = rows + dot(at[...], wo[l].reshape(1024, 1024))
            rs[...] = rows.reshape(8, 16, 1024)
            x = layer_norm(rows, gains[l, pl.ds(1, 1), :]).astype(BF16)
            part = jnp.zeros((128, 1024), F32)
            for h in range(2):
                hid = dot(x, wu[h, l])
                hid = 0.5 * hid * (1.0 + lax.erf(hid * (0.5 ** 0.5)))
                part = part + dot(hid.astype(BF16), wd[h, l])
            for c in ca:
                c.wait_send()
            cp.wait_send()
            sum_rows(part)
            return carry

        lax.fori_loop(0, LAYERS, layer_body, 0)
        fb[i] = layer_norm(resid[...], fgain[...]).astype(BF16)
        c = partner(fb.at[i], fb.at[i], 4)
        c.start()
        partner(fb.at[i], fb.at[1 - i], 4).wait_recv()
        fin = fb[...].reshape(32, 1024)
        for q in range(8):
            d = dot_t(fin, headp[q])
            st[q] = st[q] + d
            db[step, q] = d.astype(BF16)
        c.wait_send()
        for k in range(7):
            remote(db.at[step, var_dst[k]], dlr.at[step, p], s_d_s.at[step, k], s_d_r.at[step, k],
                   var_dev(var_dst[k])).start()
        dlr[step, p] = db[step, p]
        return carry

    lax.fori_loop(0, STEPS, step_body, 0)

    state = fields[:, 0, :]
    for step in range(STEPS):
        for k in range(7):
            c = remote(db.at[step, var_dst[k]], dlr.at[step, var_src[k]], s_d_s.at[step, k],
                       s_d_r.at[step, k], var_dev(var_dst[k]))
            c.wait_recv()
            c.wait_send()
        d = jnp.transpose(dlr[step].astype(F32).reshape(256, 128))
        state = state + d[:48]
        out[step] = state.reshape(48, 1, 256)


def per_device(
    fields, channel_ids, lead_index, embed_weight, var_table, agg_query, agg_kv, agg_out,
    agg_temp, pos_table, lead_table, norm_gain, qkv_weight, attn_temp, out_weight,
    up_weight, down_weight, final_gain, head_weight,
):
    vm = pl.BlockSpec(memory_space=pltpu.VMEM)
    sm = pl.BlockSpec(memory_space=pltpu.SMEM)
    hb = pl.BlockSpec(memory_space=pl.ANY)
    dma = pltpu.SemaphoreType.DMA
    V = pltpu.VMEM
    qkv_t = jnp.transpose(qkv_weight, (0, 2, 3, 1)).reshape(LAYERS, 192, 1024)
    head_t = jnp.transpose(head_weight, (1, 2, 0)).reshape(8, 2, 48, 1024)
    out = pl.pallas_call(
        kernel,
        out_shape=jax.ShapeDtypeStruct((STEPS, 48, 1, 256), F32),
        in_specs=[sm] * 3 + [hb] * 16,
        out_specs=vm,
        scratch_shapes=[
            V((48, 1, 256), F32),
            V((48, 1024), BF16),
            V((16, 64), BF16),
            V((1, 16), F32),
            V((16, 1024), BF16),
            V((LAYERS, 2, 1024), F32),
            V((1, 1024), F32),
            V((1024, 2, 1024), BF16),
            V((2, LAYERS, 128, 1024), BF16),
            V((2, LAYERS, 128, 1024), BF16),
            V((LAYERS, 16, 64, 1024), BF16),
            V((2, LAYERS, 1024, 256), BF16),
            V((2, LAYERS, 256, 1024), BF16),
            V((1024, 2048), BF16),
            V((1024, 1024), BF16),
            V((8, 128, 1024), BF16),
            V((16, 1024), BF16),
            V((8, 32, 128), F32),
            V((8, 32, 128), F32),
            V((8, 48, 1024), BF16),
            V((8, 64, 2048), BF16),
            V((8, 96, 1024), BF16),
            V((8, 96, 1024), BF16),
            V((8, 96, 1024), BF16),
            V((8, 96, 128), BF16),
            V((2, 16, 2048), F32),
            V((16, 2048), F32),
            V((128, 1024), BF16),
            V((128, 1024), BF16),
            V((16, 1024), F32),
            V((8, 16, 1024), BF16),
            V((8, 16, 1024), BF16),
            V((7, 16, 1024), BF16),
            V((2, 128, 128), BF16),
            V((2, 128, 128), BF16),
            V((LAYERS, 8, 2, 128, 128), BF16),
            V((2, 128, 128), BF16),
            V((2, 64, 128), BF16),
            V((16, 64, 128), BF16),
            V((128, 1024), BF16),
            V((8, 16, 1024), F32),
            V((2, 16, 1024), BF16),
            V((STEPS, 8, 32, 128), BF16),
            V((STEPS, 8, 32, 128), BF16),
            dma((17,)),
            dma((5,)), dma((5,)),
            dma((7,)), dma((7,)),
            dma((7,)), dma((7,)),
            dma((7,)), dma((7,)),
            dma((7,)), dma((7,)),
            dma((14,)), dma((LAYERS, 14)),
            dma((5,)), dma((5,)),
            dma((STEPS, 7)), dma((STEPS, 7)),
            dma((14,)), dma((14,)),
            dma((LAYERS, 7)), dma((LAYERS, 7)),
            dma((LAYERS, 7)), dma((LAYERS, 7)),
        ],
        compiler_params=pltpu.CompilerParams(
            collective_id=0, has_side_effects=True, vmem_limit_bytes=60 * 1024 * 1024
        ),
        name="rollout",
    )(
        channel_ids,
        lead_index,
        attn_temp.reshape(LAYERS),
        fields.reshape(48, 1, 256),
        embed_weight.reshape(48, 1024),
        var_table,
        agg_query,
        agg_kv,
        agg_out,
        agg_temp.reshape(1, 16),
        pos_table,
        lead_table,
        norm_gain,
        qkv_t,
        out_weight.reshape(LAYERS, 64, 1024),
        up_weight,
        down_weight,
        final_gain.reshape(1, 1024),
        head_t,
    )
    return out.reshape(STEPS, 3, 16, 1, 256)


def solution(mesh):
    return jax.shard_map(
        per_device,
        mesh=mesh,
        in_specs=(
            P("var", None, None, "seq"),
            P("var"),
            P(),
            P("var", None, None),
            P(),
            P(),
            P(),
            P(),
            P(),
            P("seq", None),
            P(),
            P(),
            P(None, None, "var", None),
            P(None, "var"),
            P(None, "var", None, None),
            P(None, None, "var"),
            P(None, "var", None),
            P(),
            P(),
        ),
        out_specs=P(None, "var", None, None, "seq"),
        check_vma=False,
    )
```

```python
import jax
import jax.numpy as jnp
from jax import lax
from jax.experimental import pallas as pl
from jax.experimental.pallas import tpu as pltpu
from jax.sharding import PartitionSpec as P

STEPS = 2
LAYERS = 2
EPS_NORM = 1e-05
EPS_UNIT = 1e-06
F32 = jnp.float32
BF16 = jnp.bfloat16
MESH = pl.DeviceIdType.MESH

VAR_OFFS = ((2, 1), (1, 1), (3, 1), (2, 0), (0, 1), (1, 0), (3, 0))
SEQ_OFFS = ((2, 1), (1, 1), (3, 1), (0, 1), (2, 0), (1, 0), (3, 0))


def dot(a, b):
    return lax.dot_general(a, b, (((1,), (0,)), ((), ())), preferred_element_type=F32)


def dot_t(a, b):
    return lax.dot_general(a, b, (((1,), (1,)), ((), ())), preferred_element_type=F32)


def layer_norm(values, gain):
    centre = values - jnp.mean(values, axis=-1, keepdims=True)
    spread = jnp.mean(centre * centre, axis=-1, keepdims=True)
    return centre * lax.rsqrt(spread + EPS_NORM) * gain


def kernel(
    ids, lead, temp, fields_h, emb, vart_h, aquery_h, kv_h, aout_h, atemp_h, pos_h, leadt_h, gains_h,
    qkv_h, wo_h, up_h, dn_h, fgain_h, head_h,
    out,
    fields, vart, aquery, atemp, leadt, gains, fgain, kv3,
    wq, wkv, wo, wu, wd, kvv, aout, headp, posv,
    fsnd, st, we, mb, kb, k2, vv, wb, ndx, ndr, hexp, qexp,
    resid, xg, pb, rsb, qb, qx, kvb, kvo, ax, ab, at, rs, fb, db, dlr,
    s_loc, s_ws, s_wr, s_is, s_ir, s_es, s_er, s_ag_s, s_ag_r, s_rs_s, s_rs_r,
    s_kv_s, s_kv_r, s_px_s, s_px_r, s_d_s, s_d_r,
    s_at_s, s_at_r, s_wo_s, s_wo_r, s_wz_s, s_wz_r, s_wp_s, s_wp_r,
):
    s = lax.axis_index("seq")
    v = lax.axis_index("var")
    i = v % 2
    p = v // 2
    px = p % 4
    py = p // 4
    sz = s // 2
    sy = s % 2
    other = (s, p * 2 + (1 - i))

    var_dst = []
    var_src = []
    for dx, dy in VAR_OFFS:
        var_dst.append(((py + dy) % 2) * 4 + (px + dx) % 4)
        var_src.append(((py + 2 - dy) % 2) * 4 + (px + 4 - dx) % 4)
    seq_dst = []
    seq_src = []
    for dz, dy in SEQ_OFFS:
        seq_dst.append(((sz + dz) % 4) * 2 + (sy + dy) % 2)
        seq_src.append(((sz + 4 - dz) % 4) * 2 + (sy + 2 - dy) % 2)

    def var_dev(q):
        return (s, q * 2 + i)

    def remote(src, dst, send, recv, dev):
        return pltpu.make_async_remote_copy(
            src_ref=src, dst_ref=dst, send_sem=send, recv_sem=recv, device_id=dev, device_id_type=MESH
        )

    own_heads = ((qkv_h.at[:, pl.ds(0, 64)], wq.at[i, :, pl.ds(0, 64)]),
                 (qkv_h.at[:, pl.ds(64, 128)], wkv.at[i]),
                 (up_h, wu.at[i]),
                 (dn_h, wd.at[i]))
    mine = pl.ds(sz * 16, 16)
    loads = []
    for k, (a, b) in enumerate((
        (fields_h, fields), (kv_h, kv3), (emb, we.at[p]), (aquery_h, aquery), (vart_h, vart), (atemp_h, atemp),
        (aout_h, aout), (pos_h.at[pl.ds(v * 16, 16)], posv), (leadt_h, leadt), (gains_h, gains),
        (fgain_h, fgain), (head_h.at[:, i], headp.at[:, pl.ds(0, 48)]), *own_heads, (wo_h.at[:, mine], wo.at[:, p, i, mine]),
    )):
        loads.append(pltpu.make_async_copy(a, b, s_loc.at[k]))
    for c in loads[:6]:
        c.start()

    bar = pltpu.get_barrier_semaphore()
    for q in var_dst:
        for j in range(2):
            pl.semaphore_signal(bar, inc=1, device_id=(s, q * 2 + j), device_id_type=MESH)
    for t in seq_dst:
        for j in range(2):
            pl.semaphore_signal(bar, inc=1, device_id=(t, p * 2 + j), device_id_type=MESH)
    pl.semaphore_signal(bar, inc=1, device_id=other, device_id_type=MESH)

    for c in loads[6:]:
        c.start()
    loads[0].wait()
    state0 = fields[:, 0, :]
    frow = lax.broadcasted_iota(jnp.int32, (80, 256), 0)
    fcol = lax.broadcasted_iota(jnp.int32, (80, 256), 1) % 32
    named = jnp.where(fcol == 0, ids[0], jnp.where(fcol == 1, ids[1], jnp.where(fcol == 2, ids[2], 0)))
    extra = jnp.where(frow == 0, named, 0).astype(F32)
    fsnd[...] = jnp.transpose(jnp.concatenate([state0, extra], axis=0)).reshape(8, 32, 128)

    pl.semaphore_wait(bar, 29)

    init = []
    for k in range(7):
        init.append(remote(fsnd.at[var_dst[k]], st.at[p], s_is.at[k], s_ir.at[k], var_dev(var_dst[k])))
        init.append(remote(emb, we.at[p], s_es.at[k], s_er.at[k], var_dev(var_dst[k])))
    for c in init:
        c.start()
    wcopies = []
    for k, (a, b) in enumerate(own_heads):
        wcopies.append(remote(a, b, s_ws.at[k], s_wr.at[k], other))
    for c in wcopies:
        c.start()

    def wo_copy(l, k):
        return remote(wo_h.at[l, mine], wo.at[l, p, i, mine], s_wo_s.at[l, k], s_wo_r.at[l, k], var_dev(var_dst[k]))

    def wo_arrival(l, k):
        return remote(wo_h.at[l, mine], wo.at[l, var_src[k], i, mine], s_wo_s.at[l, k], s_wo_r.at[l, k],
                      var_dev(var_dst[k]))

    def wo_quarter(l, dz, back):
        rows = pl.ds(((sz + 4 - dz) % 4) * 16, 16) if back else mine
        quarter = wo.at[l, :, i, rows]
        return remote(quarter, quarter, s_wz_s.at[l, dz - 1], s_wz_r.at[l, dz - 1], (((sz + dz) % 4) * 2 + sy, v))

    def wo_pass(l, core):
        return remote(wo.at[l, :, core], wo.at[l, :, core], s_wp_s.at[l], s_wp_r.at[l], other)

    def wo_spread(l):
        for k in range(7):
            wo_arrival(l, k).wait_recv()
        for dz in (2, 1, 3):
            wo_quarter(l, dz, False).start()

    for k in range(7):
        wo_copy(0, k).start()

    st[p] = fsnd[p]
    wq[:, :, pl.ds(64, 64)] = jnp.zeros((2, LAYERS, 64, 1024), BF16)
    headp[:, pl.ds(48, 80)] = jnp.zeros((8, 80, 1024), BF16)

    hrow = lax.broadcasted_iota(jnp.int32, (128, 1024), 0)
    hcol = lax.broadcasted_iota(jnp.int32, (128, 1024), 1) // 64
    hexp[...] = jnp.where(hrow == hcol, 1.0, 0.0).astype(BF16)
    loads[3].wait()
    aq = aquery[...].astype(F32)
    aq = aq * lax.rsqrt(jnp.mean(aq * aq, axis=-1, keepdims=True) + EPS_UNIT)
    aqt = jnp.concatenate([aq] * 16, axis=1)
    aqt = jnp.concatenate([aqt, jnp.zeros((112, 1024), F32)], axis=0)
    qexp[...] = jnp.where(hrow == hcol, aqt, 0.0).astype(BF16)
    for c in loads[4:6]:
        c.wait()
    tvec = jnp.concatenate([atemp[...] * (1.0 / 64.0), jnp.zeros((1, 112), F32)], axis=1)

    loads[1].wait()

    def split_kv(n, c):
        rows = pl.ds(n * 64, 64)
        kvv[rows] = kv3[rows].reshape(64, 2048)
        return c

    lax.fori_loop(0, 16, split_kv, 0)
    loads[2].wait()
    for k in range(7):
        remote(fsnd.at[0], st.at[var_src[k]], s_is.at[k], s_ir.at[k], var_dev(var_dst[k])).wait_recv()
    nrow = lax.broadcasted_iota(jnp.int32, (128, 48), 0) % 16
    ncol = lax.broadcasted_iota(jnp.int32, (128, 48), 1).astype(F32)
    named = st[:, pl.ds(0, 16)].reshape(128, 128)[:, 48:49]
    hot = jnp.where((named == ncol) & (nrow < 3), 1.0, 0.0).astype(BF16)
    vall = dot(hot, vart[...]).astype(BF16)
    for n in range(4):
        cols = pl.ds(n * 512, 512)
        mb[:, pl.ds(48, 16), cols] = dot(vall, kvv[:, cols]).astype(BF16).reshape(8, 16, 512)
    for k in range(7):
        remote(emb, we.at[var_src[k]], s_es.at[k], s_er.at[k], var_dev(var_dst[k])).wait_recv()
    wall = we[...].reshape(384, 1024)
    for n in range(4):
        cols = pl.ds(n * 512, 512)
        mb[:, pl.ds(0, 48), cols] = dot(wall, kvv[:, cols]).astype(BF16).reshape(8, 48, 512)
    for c in init:
        c.wait_send()
    for c in loads[6:12]:
        c.wait()
    loads[16].wait()
    wo_spread(0)

    lane64 = lax.broadcasted_iota(jnp.int32, (32, 64), 1)
    lane128 = lax.broadcasted_iota(jnp.int32, (128, 128), 1)

    def partner(src, dst, k):
        return remote(src, dst, s_px_s.at[k], s_px_r.at[k], other)

    def gather_rows(own):
        xg[p] = own.astype(BF16)
        cs = [remote(xg.at[p], xg.at[p], s_ag_s.at[k], s_ag_r.at[k], var_dev(var_dst[k])) for k in range(7)]
        for c in cs:
            c.start()
        for k in range(7):
            remote(xg.at[p], xg.at[var_src[k]], s_ag_s.at[k], s_ag_r.at[k], var_dev(var_dst[k])).wait_recv()
        return xg[...].reshape(128, 1024), cs

    def sum_rows(part):
        pb[...] = part.astype(BF16).reshape(8, 16, 1024)
        cs = [remote(pb.at[var_dst[k]], rsb.at[k], s_rs_s.at[k], s_rs_r.at[k], var_dev(var_dst[k])) for k in range(7)]
        for c in cs:
            c.start()
        total = rs[p] + pb[p].astype(F32)
        for k in (6, 5, 4, 3, 2, 1, 0):
            cs[k].wait_recv()
            total = total + rsb[k].astype(F32)
        resid[...] = total
        for c in cs:
            c.wait_send()

    def step_body(step, carry):
        for q in range(8):
            sb = st[q][:, :64]
            blk = jnp.concatenate(
                [jnp.where(lane64 // 16 == n, sb, jnp.where(lane64 == 48 + n, 1.0, 0.0)) for n in range(3)], axis=0
            ).astype(BF16)
            kk = dot(blk, mb[q, :, pl.ds(0, 1024)])
            kb[q] = kk.astype(BF16)
            k2[q] = (kk * kk).astype(BF16)
            vv[q] = dot(blk, mb[q, :, pl.ds(1024, 1024)]).astype(BF16)
        ss = dot_t(k2[...].reshape(768, 1024), hexp[...])
        qk = dot_t(kb[...].reshape(768, 1024), qexp[...])
        w = jnp.exp(qk * lax.rsqrt(ss * (1.0 / 64.0) + EPS_UNIT) * tvec)
        wb[...] = w.astype(BF16).reshape(8, 96, 128)
        num = jnp.zeros((32, 1024), F32)
        den = jnp.zeros((32, 1024), F32)
        for q in range(8):
            wx = dot(wb[q], hexp[...])
            nx = wx * vv[q].astype(F32)
            num = num + (nx[0:32] + nx[32:64] + nx[64:96])
            den = den + (wx[0:32] + wx[32:64] + wx[64:96])
        ndx[:, :, pl.ds(0, 1024)] = num.reshape(2, 16, 1024)
        ndx[:, :, pl.ds(1024, 1024)] = den.reshape(2, 16, 1024)
        c = partner(ndx.at[1 - i], ndr, 0)
        c.start()
        row16 = lax.broadcasted_iota(jnp.int32, (16, 16), 1)
        lhot = jnp.where(row16 == lead[0] + step, 1.0, 0.0).astype(BF16)
        add = posv[...].astype(F32) + dot(lhot, leadt[...])
        c.wait_recv()
        tot = ndx[i] + ndr[...]
        pooled = (tot[:, :1024] / tot[:, 1024:]).astype(BF16)
        c.wait_send()
        resid[...] = dot(pooled, aout[...]) + add

        @pl.when(step == 0)
        def _():
            for c in loads[12:16]:
                c.wait()
            for c in wcopies:
                c.wait()

        def layer_body(l, carry):
            x, cg = gather_rows(resid[...])

            rows = x.astype(F32)
            x = layer_norm(rows, gains[l, pl.ds(0, 1), :]).astype(BF16)
            cs = []
            for h in range(2):
                kv = dot_t(x, wkv[h, l])
                kq = jnp.where(lane128 < 64, kv * kv, 0.0)
                scale = lax.rsqrt(jnp.sum(kq, axis=-1, keepdims=True) * (1.0 / 64.0) + EPS_UNIT)
                kvo[h] = (kv * jnp.where(lane128 < 64, scale, 1.0)).astype(BF16)
                for k in range(7):
                    c = remote(kvo.at[h], kvb.at[l, s, i], s_kv_s.at[2 * k + h],
                               s_kv_r.at[l, 2 * k + i], (seq_dst[k], p * 2 + h))
                    c.start()
                    cs.append(c)
            ck = partner(kvo.at[1 - i], kvb.at[l, s, i], 2)
            ck.start()

            @pl.when((step == 0) & (l == 0))
            def _():
                for k in range(7):
                    wo_copy(1, k).start()

            for h in range(2):
                q = dot_t(x, wq[h, l])
                q = q * lax.rsqrt(jnp.sum(q * q, axis=-1, keepdims=True) * (1.0 / 64.0) + EPS_UNIT)
                qx[h] = q.astype(BF16)
            cq = partner(qx.at[1 - i], qb.at[i], 1)
            cq.start()
            qb[i] = qx[i]
            kvb[l, s, i] = kvo[i]

            @pl.when(step == 0)
            def _():
                for dz in (1, 2, 3):
                    wo_quarter(l, dz, True).wait_recv()
                wo_pass(l, i).start()

            for c in cg:
                c.wait_send()
            partner(qx.at[1 - i], qb.at[1 - i], 1).wait_recv()
            partner(kvo.at[1 - i], kvb.at[l, s, 1 - i], 2).wait_recv()
            scale = temp[l] * (1.0 / 64.0)
            q = qb[...].reshape(256, 128)
            num = jnp.zeros((256, 128), F32)
            den = jnp.zeros((256, 128), F32)
            for k in (7, 6, 5, 4, 3, 2, 1, 0):
                if k == 7:
                    src = s
                else:
                    src = seq_src[k]
                    for j in range(2):
                        remote(kvo.at[j], kvb.at[l, src, j], s_kv_s.at[2 * k + j],
                               s_kv_r.at[l, 2 * k + j], (seq_dst[k], p * 2 + j)).wait_recv()
                kv = kvb[l, src].reshape(256, 128)
                e = jnp.exp(dot_t(q, kv) * scale)
                den = den + e[:, :128] + e[:, 128:]
                num = num + dot(e.astype(BF16), kv)
            att = num / jnp.sum(den, axis=-1, keepdims=True)
            for h in range(2):
                lo, hi = att[128 * h : 128 * h + 64], att[128 * h + 64 : 128 * h + 128]
                ax[h] = jnp.where(lane128[:64] < 64, pltpu.roll(lo, 64, 1), hi).astype(BF16)
            ca = []
            for k in range(7):
                for j in range(2):
                    ca.append(remote(ax.at[j], ab.at[v], s_at_s.at[2 * k + j], s_at_r.at[2 * k + i],
                                     (s, var_dst[k] * 2 + j)))
            for c in ca:
                c.start()
            cp = partner(ax.at[1 - i], ab.at[v], 3)
            cp.start()
            ab[v] = ax[i]
            for c in cs:
                c.wait_send()
            cq.wait_send()
            ck.wait_send()

            @pl.when(step == 0)
            def _():
                wo_pass(l, 1 - i).wait_recv()
                wo_pass(l, i).wait_send()
                for k in range(7):
                    wo_copy(l, k).wait_send()
                for dz in (1, 2, 3):
                    wo_quarter(l, dz, False).wait_send()

            partner(ax.at[1 - i], ab.at[p * 2 + 1 - i], 3).wait_recv()
            for k in range(7):
                for j in range(2):
                    remote(ax.at[j], ab.at[var_src[k] * 2 + j], s_at_s.at[2 * k + j], s_at_r.at[2 * k + j],
                           (s, var_dst[k] * 2 + j)).wait_recv()
            for q in range(8):
                even, odd = ab[2 * q].astype(F32), ab[2 * q + 1].astype(F32)
                cols = pl.ds(q * 128, 128)
                left = lane128[:64] < 64
                at[pl.ds(0, 64), cols] = jnp.where(left, even, pltpu.roll(odd, 64, 1)).astype(BF16)
                at[pl.ds(64, 64), cols] = jnp.where(left, pltpu.roll(even, 64, 1), odd).astype(BF16)
            rows = rows + dot(at[...], wo[l].reshape(1024, 1024))
            rs[...] = rows.reshape(8, 16, 1024)

            @pl.when((step == 0) & (l == 0))
            def _():
                wo_spread(1)

            x = layer_norm(rows, gains[l, pl.ds(1, 1), :]).astype(BF16)
            part = jnp.zeros((128, 1024), F32)
            for h in range(2):
                hid = dot(x, wu[h, l])
                hid = 0.5 * hid * (1.0 + lax.erf(hid * (0.5 ** 0.5)))
                part = part + dot(hid.astype(BF16), wd[h, l])
            for c in ca:
                c.wait_send()
            cp.wait_send()
            sum_rows(part)
            return carry

        lax.fori_loop(0, LAYERS, layer_body, 0)
        fb[i] = layer_norm(resid[...], fgain[...]).astype(BF16)
        c = partner(fb.at[i], fb.at[i], 4)
        c.start()
        partner(fb.at[i], fb.at[1 - i], 4).wait_recv()
        fin = fb[...].reshape(32, 1024)
        for q in range(8):
            d = dot_t(fin, headp[q])
            st[q] = st[q] + d
            db[step, q] = d.astype(BF16)
        c.wait_send()
        for k in range(7):
            remote(db.at[step, var_dst[k]], dlr.at[step, p], s_d_s.at[step, k], s_d_r.at[step, k],
                   var_dev(var_dst[k])).start()
        dlr[step, p] = db[step, p]
        return carry

    lax.fori_loop(0, STEPS, step_body, 0)

    state = fields[:, 0, :]
    for step in range(STEPS):
        for k in range(7):
            c = remote(db.at[step, var_dst[k]], dlr.at[step, var_src[k]], s_d_s.at[step, k],
                       s_d_r.at[step, k], var_dev(var_dst[k]))
            c.wait_recv()
            c.wait_send()
        d = jnp.transpose(dlr[step].astype(F32).reshape(256, 128))
        state = state + d[:48]
        out[step] = state.reshape(48, 1, 256)


def per_device(
    fields, channel_ids, lead_index, embed_weight, var_table, agg_query, agg_kv, agg_out,
    agg_temp, pos_table, lead_table, norm_gain, qkv_weight, attn_temp, out_weight,
    up_weight, down_weight, final_gain, head_weight,
):
    vm = pl.BlockSpec(memory_space=pltpu.VMEM)
    sm = pl.BlockSpec(memory_space=pltpu.SMEM)
    hb = pl.BlockSpec(memory_space=pl.ANY)
    dma = pltpu.SemaphoreType.DMA
    V = pltpu.VMEM
    qkv_t = jnp.transpose(qkv_weight, (0, 2, 3, 1)).reshape(LAYERS, 192, 1024)
    head_t = jnp.transpose(head_weight, (1, 2, 0)).reshape(8, 2, 48, 1024)
    out = pl.pallas_call(
        kernel,
        out_shape=jax.ShapeDtypeStruct((STEPS, 48, 1, 256), F32),
        in_specs=[sm] * 3 + [hb] * 16,
        out_specs=vm,
        scratch_shapes=[
            V((48, 1, 256), F32),
            V((48, 1024), BF16),
            V((16, 64), BF16),
            V((1, 16), F32),
            V((16, 1024), BF16),
            V((LAYERS, 2, 1024), F32),
            V((1, 1024), F32),
            V((1024, 2, 1024), BF16),
            V((2, LAYERS, 128, 1024), BF16),
            V((2, LAYERS, 128, 1024), BF16),
            V((LAYERS, 8, 2, 64, 1024), BF16),
            V((2, LAYERS, 1024, 256), BF16),
            V((2, LAYERS, 256, 1024), BF16),
            V((1024, 2048), BF16),
            V((1024, 1024), BF16),
            V((8, 128, 1024), BF16),
            V((16, 1024), BF16),
            V((8, 32, 128), F32),
            V((8, 32, 128), F32),
            V((8, 48, 1024), BF16),
            V((8, 64, 2048), BF16),
            V((8, 96, 1024), BF16),
            V((8, 96, 1024), BF16),
            V((8, 96, 1024), BF16),
            V((8, 96, 128), BF16),
            V((2, 16, 2048), F32),
            V((16, 2048), F32),
            V((128, 1024), BF16),
            V((128, 1024), BF16),
            V((16, 1024), F32),
            V((8, 16, 1024), BF16),
            V((8, 16, 1024), BF16),
            V((7, 16, 1024), BF16),
            V((2, 128, 128), BF16),
            V((2, 128, 128), BF16),
            V((LAYERS, 8, 2, 128, 128), BF16),
            V((2, 128, 128), BF16),
            V((2, 64, 128), BF16),
            V((16, 64, 128), BF16),
            V((128, 1024), BF16),
            V((8, 16, 1024), F32),
            V((2, 16, 1024), BF16),
            V((STEPS, 8, 32, 128), BF16),
            V((STEPS, 8, 32, 128), BF16),
            dma((17,)),
            dma((5,)), dma((5,)),
            dma((7,)), dma((7,)),
            dma((7,)), dma((7,)),
            dma((7,)), dma((7,)),
            dma((7,)), dma((7,)),
            dma((14,)), dma((LAYERS, 14)),
            dma((5,)), dma((5,)),
            dma((STEPS, 7)), dma((STEPS, 7)),
            dma((14,)), dma((14,)),
            dma((LAYERS, 7)), dma((LAYERS, 7)),
            dma((LAYERS, 3)), dma((LAYERS, 3)),
            dma((LAYERS,)), dma((LAYERS,)),
        ],
        compiler_params=pltpu.CompilerParams(
            collective_id=0, has_side_effects=True, vmem_limit_bytes=60 * 1024 * 1024
        ),
        name="rollout",
    )(
        channel_ids,
        lead_index,
        attn_temp.reshape(LAYERS),
        fields.reshape(48, 1, 256),
        embed_weight.reshape(48, 1024),
        var_table,
        agg_query,
        agg_kv,
        agg_out,
        agg_temp.reshape(1, 16),
        pos_table,
        lead_table,
        norm_gain,
        qkv_t,
        out_weight.reshape(LAYERS, 64, 1024),
        up_weight,
        down_weight,
        final_gain.reshape(1, 1024),
        head_t,
    )
    return out.reshape(STEPS, 3, 16, 1, 256)


def solution(mesh):
    return jax.shard_map(
        per_device,
        mesh=mesh,
        in_specs=(
            P("var", None, None, "seq"),
            P("var"),
            P(),
            P("var", None, None),
            P(),
            P(),
            P(),
            P(),
            P(),
            P("seq", None),
            P(),
            P(),
            P(None, None, "var", None),
            P(None, "var"),
            P(None, "var", None, None),
            P(None, None, "var"),
            P(None, "var", None),
            P(),
            P(),
        ),
        out_specs=P(None, "var", None, None, "seq"),
        check_vma=False,
    )
```

```python
import jax
import jax.numpy as jnp
from jax import lax
from jax.experimental import pallas as pl
from jax.experimental.pallas import tpu as pltpu
from jax.sharding import PartitionSpec as P

STEPS = 2
LAYERS = 2
EPS_NORM = 1e-05
EPS_UNIT = 1e-06
F32 = jnp.float32
BF16 = jnp.bfloat16
MESH = pl.DeviceIdType.MESH

VAR_OFFS = ((2, 1), (1, 1), (3, 1), (2, 0), (0, 1), (1, 0), (3, 0))
SEQ_OFFS = ((2, 1), (1, 1), (3, 1), (0, 1), (2, 0), (1, 0), (3, 0))


def dot(a, b):
    return lax.dot_general(a, b, (((1,), (0,)), ((), ())), preferred_element_type=F32)


def dot_t(a, b):
    return lax.dot_general(a, b, (((1,), (1,)), ((), ())), preferred_element_type=F32)


def layer_norm(values, gain):
    centre = values - jnp.mean(values, axis=-1, keepdims=True)
    spread = jnp.mean(centre * centre, axis=-1, keepdims=True)
    return centre * lax.rsqrt(spread + EPS_NORM) * gain


def kernel(
    ids, lead, temp, fields_h, emb, vart_h, aquery_h, kv_h, aout_h, atemp_h, pos_h, leadt_h, gains_h,
    qkv_h, wo_h, up_h, dn_h, fgain_h, head_h,
    out,
    fields, vart, aquery, atemp, leadt, gains, fgain, kv3,
    wq, wkv, wo, wu, wd, kvv, aout, headp, posv,
    fsnd, st, we, mb, kb, k2, vv, wb, ndx, ndr, hexp, qexp,
    resid, xg, pb, rsb, qb, qx, kvb, kvo, ax, ab, at, rs, fb, db, dlr,
    s_loc, s_ws, s_wr, s_is, s_ir, s_es, s_er, s_ag_s, s_ag_r, s_rs_s, s_rs_r,
    s_kv_s, s_kv_r, s_px_s, s_px_r, s_d_s, s_d_r,
    s_at_s, s_at_r, s_wo_s, s_wo_r, s_wz_s, s_wz_r, s_wp_s, s_wp_r,
):
    s = lax.axis_index("seq")
    v = lax.axis_index("var")
    i = v % 2
    p = v // 2
    px = p % 4
    py = p // 4
    sz = s // 2
    sy = s % 2
    other = (s, p * 2 + (1 - i))

    var_dst = []
    var_src = []
    for dx, dy in VAR_OFFS:
        var_dst.append(((py + dy) % 2) * 4 + (px + dx) % 4)
        var_src.append(((py + 2 - dy) % 2) * 4 + (px + 4 - dx) % 4)
    seq_dst = []
    seq_src = []
    for dz, dy in SEQ_OFFS:
        seq_dst.append(((sz + dz) % 4) * 2 + (sy + dy) % 2)
        seq_src.append(((sz + 4 - dz) % 4) * 2 + (sy + 2 - dy) % 2)

    def var_dev(q):
        return (s, q * 2 + i)

    def remote(src, dst, send, recv, dev):
        return pltpu.make_async_remote_copy(
            src_ref=src, dst_ref=dst, send_sem=send, recv_sem=recv, device_id=dev, device_id_type=MESH
        )

    own_heads = ((qkv_h.at[:, pl.ds(0, 64)], wq.at[:, i, pl.ds(0, 64)]),
                 (qkv_h.at[:, pl.ds(64, 128)], wkv.at[:, i]),
                 (up_h, wu.at[i]),
                 (dn_h, wd.at[i]))
    mine = pl.ds(sz * 16, 16)
    loads = []
    for k, (a, b) in enumerate((
        (fields_h, fields), (kv_h, kv3), (emb, we.at[p]), (aquery_h, aquery), (vart_h, vart), (atemp_h, atemp),
        (aout_h, aout), (pos_h.at[pl.ds(v * 16, 16)], posv), (leadt_h, leadt), (gains_h, gains),
        (fgain_h, fgain), (head_h.at[:, i], headp.at[:, pl.ds(0, 48)]), *own_heads, (wo_h.at[:, mine], wo.at[:, p, i, mine]),
    )):
        loads.append(pltpu.make_async_copy(a, b, s_loc.at[k]))
    for c in loads[:6]:
        c.start()

    bar = pltpu.get_barrier_semaphore()
    for q in var_dst:
        for j in range(2):
            pl.semaphore_signal(bar, inc=1, device_id=(s, q * 2 + j), device_id_type=MESH)
    for t in seq_dst:
        for j in range(2):
            pl.semaphore_signal(bar, inc=1, device_id=(t, p * 2 + j), device_id_type=MESH)
    pl.semaphore_signal(bar, inc=1, device_id=other, device_id_type=MESH)

    for c in loads[6:]:
        c.start()
    loads[0].wait()
    state0 = fields[:, 0, :]
    frow = lax.broadcasted_iota(jnp.int32, (80, 256), 0)
    fcol = lax.broadcasted_iota(jnp.int32, (80, 256), 1) % 32
    named = jnp.where(fcol == 0, ids[0], jnp.where(fcol == 1, ids[1], jnp.where(fcol == 2, ids[2], 0)))
    extra = jnp.where(frow == 0, named, 0).astype(F32)
    fsnd[...] = jnp.transpose(jnp.concatenate([state0, extra], axis=0)).reshape(8, 32, 128)

    pl.semaphore_wait(bar, 29)

    init = []
    for k in range(7):
        init.append(remote(fsnd.at[var_dst[k]], st.at[p], s_is.at[k], s_ir.at[k], var_dev(var_dst[k])))
        init.append(remote(emb, we.at[p], s_es.at[k], s_er.at[k], var_dev(var_dst[k])))
    for c in init:
        c.start()
    wcopies = []
    for k, (a, b) in enumerate(own_heads):
        wcopies.append(remote(a, b, s_ws.at[k], s_wr.at[k], other))
    for c in wcopies:
        c.start()

    def wo_copy(l, k):
        return remote(wo_h.at[l, mine], wo.at[l, p, i, mine], s_wo_s.at[l, k], s_wo_r.at[l, k], var_dev(var_dst[k]))

    def wo_arrival(l, k):
        return remote(wo_h.at[l, mine], wo.at[l, var_src[k], i, mine], s_wo_s.at[l, k], s_wo_r.at[l, k],
                      var_dev(var_dst[k]))

    def wo_quarter(l, dz, back):
        rows = pl.ds(((sz + 4 - dz) % 4) * 16, 16) if back else mine
        quarter = wo.at[l, :, i, rows]
        return remote(quarter, quarter, s_wz_s.at[l, dz - 1], s_wz_r.at[l, dz - 1], (((sz + dz) % 4) * 2 + sy, v))

    def wo_pass(l, core):
        return remote(wo.at[l, :, core], wo.at[l, :, core], s_wp_s.at[l], s_wp_r.at[l], other)

    def wo_spread(l):
        for k in range(7):
            wo_arrival(l, k).wait_recv()
        for dz in (2, 1, 3):
            wo_quarter(l, dz, False).start()

    for k in range(7):
        wo_copy(0, k).start()

    st[p] = fsnd[p]
    wq[:, :, pl.ds(64, 64)] = jnp.zeros((LAYERS, 2, 64, 1024), BF16)
    headp[:, pl.ds(48, 80)] = jnp.zeros((8, 80, 1024), BF16)

    hrow = lax.broadcasted_iota(jnp.int32, (128, 1024), 0)
    hcol = lax.broadcasted_iota(jnp.int32, (128, 1024), 1) // 64
    hexp[...] = jnp.where(hrow == hcol, 1.0, 0.0).astype(BF16)
    loads[3].wait()
    aq = aquery[...].astype(F32)
    aq = aq * lax.rsqrt(jnp.mean(aq * aq, axis=-1, keepdims=True) + EPS_UNIT)
    aqt = jnp.concatenate([aq] * 16, axis=1)
    aqt = jnp.concatenate([aqt, jnp.zeros((112, 1024), F32)], axis=0)
    qexp[...] = jnp.where(hrow == hcol, aqt, 0.0).astype(BF16)
    for c in loads[4:6]:
        c.wait()
    tvec = jnp.concatenate([atemp[...] * (1.0 / 64.0), jnp.zeros((1, 112), F32)], axis=1)

    loads[1].wait()

    def split_kv(n, c):
        rows = pl.ds(n * 64, 64)
        kvv[rows] = kv3[rows].reshape(64, 2048)
        return c

    lax.fori_loop(0, 16, split_kv, 0)
    loads[2].wait()
    for k in range(7):
        remote(fsnd.at[0], st.at[var_src[k]], s_is.at[k], s_ir.at[k], var_dev(var_dst[k])).wait_recv()
    nrow = lax.broadcasted_iota(jnp.int32, (128, 48), 0) % 16
    ncol = lax.broadcasted_iota(jnp.int32, (128, 48), 1).astype(F32)
    named = st[:, pl.ds(0, 16)].reshape(128, 128)[:, 48:49]
    hot = jnp.where((named == ncol) & (nrow < 3), 1.0, 0.0).astype(BF16)
    vall = dot(hot, vart[...]).astype(BF16)
    for n in range(4):
        cols = pl.ds(n * 512, 512)
        mb[:, pl.ds(48, 16), cols] = dot(vall, kvv[:, cols]).astype(BF16).reshape(8, 16, 512)
    for k in range(7):
        remote(emb, we.at[var_src[k]], s_es.at[k], s_er.at[k], var_dev(var_dst[k])).wait_recv()
    wall = we[...].reshape(384, 1024)
    for n in range(4):
        cols = pl.ds(n * 512, 512)
        mb[:, pl.ds(0, 48), cols] = dot(wall, kvv[:, cols]).astype(BF16).reshape(8, 48, 512)
    for c in init:
        c.wait_send()
    for c in loads[6:12]:
        c.wait()
    loads[16].wait()
    wo_spread(0)

    lane64 = lax.broadcasted_iota(jnp.int32, (32, 64), 1)
    left64 = lax.broadcasted_iota(jnp.int32, (64, 128), 1) < 64

    def partner(src, dst, k):
        return remote(src, dst, s_px_s.at[k], s_px_r.at[k], other)

    def gather(c, k, src):
        return remote(xg.at[c, p], xg.at[c, src], s_ag_s.at[c, k], s_ag_r.at[c, k], var_dev(var_dst[k]))

    def start_gather(c, own):
        xg[c, p] = own.astype(BF16)
        for k in range(7):
            gather(c, k, p).start()

    def sums(c, k):
        return remote(pb.at[c, var_dst[k]], rsb.at[c, k], s_rs_s.at[c, k], s_rs_r.at[c, k], var_dev(var_dst[k]))

    def keys_out(l, c, k, h):
        return remote(kvo.at[h, c], kvb.at[l, c, s, i], s_kv_s.at[c, 2 * k + h], s_kv_r.at[l, c, 2 * k + i],
                      (seq_dst[k], p * 2 + h))

    def keys_in(l, c, k, j):
        return remote(kvo.at[j, c], kvb.at[l, c, seq_src[k], j], s_kv_s.at[c, 2 * k + j],
                      s_kv_r.at[l, c, 2 * k + j], (seq_dst[k], p * 2 + j))

    def mixed_out(c, k, j):
        return remote(ax.at[j, c], ab.at[c, v], s_at_s.at[c, 2 * k + j], s_at_r.at[c, 2 * k + i],
                      (s, var_dst[k] * 2 + j))

    def mixed_in(c, k, j):
        return remote(ax.at[j, c], ab.at[c, var_src[k] * 2 + j], s_at_s.at[c, 2 * k + j], s_at_r.at[c, 2 * k + j],
                      (s, var_dst[k] * 2 + j))

    def step_body(step, carry):
        for q in range(8):
            sb = st[q][:, :64]
            blk = jnp.concatenate(
                [jnp.where(lane64 // 16 == n, sb, jnp.where(lane64 == 48 + n, 1.0, 0.0)) for n in range(3)], axis=0
            ).astype(BF16)
            kk = dot(blk, mb[q, :, pl.ds(0, 1024)])
            kb[q] = kk.astype(BF16)
            k2[q] = (kk * kk).astype(BF16)
            vv[q] = dot(blk, mb[q, :, pl.ds(1024, 1024)]).astype(BF16)
        ss = dot_t(k2[...].reshape(768, 1024), hexp[...])
        qk = dot_t(kb[...].reshape(768, 1024), qexp[...])
        w = jnp.exp(qk * lax.rsqrt(ss * (1.0 / 64.0) + EPS_UNIT) * tvec)
        wb[...] = w.astype(BF16).reshape(8, 96, 128)
        num = jnp.zeros((32, 1024), F32)
        den = jnp.zeros((32, 1024), F32)
        for q in range(8):
            wx = dot(wb[q], hexp[...])
            nx = wx * vv[q].astype(F32)
            num = num + (nx[0:32] + nx[32:64] + nx[64:96])
            den = den + (wx[0:32] + wx[32:64] + wx[64:96])
        ndx[:, :, pl.ds(0, 1024)] = num.reshape(2, 16, 1024)
        ndx[:, :, pl.ds(1024, 1024)] = den.reshape(2, 16, 1024)
        c = partner(ndx.at[1 - i], ndr, 0)
        c.start()
        row16 = lax.broadcasted_iota(jnp.int32, (16, 16), 1)
        lhot = jnp.where(row16 == lead[0] + step, 1.0, 0.0).astype(BF16)
        add = posv[...].astype(F32) + dot(lhot, leadt[...])
        c.wait_recv()
        tot = ndx[i] + ndr[...]
        pooled = (tot[:, :1024] / tot[:, 1024:]).astype(BF16)
        c.wait_send()
        own = dot(pooled, aout[...]) + add
        for n in range(2):
            start_gather(n, own[8 * n : 8 * n + 8])

        @pl.when(step == 0)
        def _():
            for c in loads[12:16]:
                c.wait()
            for c in wcopies:
                c.wait()

        def layer_body(l, carry):
            for n in range(2):
                for k in range(7):
                    gather(n, k, var_src[k]).wait_recv()
                x = layer_norm(xg[n].astype(F32).reshape(64, 1024), gains[l, pl.ds(0, 1), :]).astype(BF16)
                both = dot_t(x, wkv[l].reshape(256, 1024))
                for h in range(2):
                    kv = both[:, 128 * h : 128 * h + 128]
                    kq = jnp.where(left64, kv * kv, 0.0)
                    scale = lax.rsqrt(jnp.sum(kq, axis=-1, keepdims=True) * (1.0 / 64.0) + EPS_UNIT)
                    kvo[h, n] = (kv * jnp.where(left64, scale, 1.0)).astype(BF16)
                for k in range(7):
                    for h in range(2):
                        keys_out(l, n, k, h).start()
                partner(kvo.at[1 - i, n], kvb.at[l, n, s, i], 5 + n).start()
                kvb[l, n, s, i] = kvo[i, n]
                both = dot_t(x, wq[l].reshape(256, 1024))
                for h in range(2):
                    q = both[:, 128 * h : 128 * h + 128]
                    q = q * lax.rsqrt(jnp.sum(q * q, axis=-1, keepdims=True) * (1.0 / 64.0) + EPS_UNIT)
                    qx[h, n] = q.astype(BF16)
            partner(qx.at[1 - i], qb.at[i], 1).start()
            qb[i] = qx[i]

            @pl.when((step == 0) & (l == 0))
            def _():
                for k in range(7):
                    wo_copy(1, k).start()

            @pl.when(step == 0)
            def _():
                for dz in (1, 2, 3):
                    wo_quarter(l, dz, True).wait_recv()
                wo_pass(l, i).start()

            for n in range(2):
                for k in range(7):
                    gather(n, k, p).wait_send()
            partner(qx.at[1 - i], qb.at[1 - i], 1).wait_recv()
            scale = temp[l] * (1.0 / 64.0)
            q = qb[...].reshape(256, 128)
            num = jnp.zeros((256, 128), F32)
            den = jnp.zeros((256, 128), F32)
            for n in range(2):
                for pair in ((7, 6), (5, 4), (3, 2), (1, 0)):
                    block = []
                    for k in pair:
                        if k == 7:
                            partner(kvo.at[1 - i, n], kvb.at[l, n, s, 1 - i], 5 + n).wait_recv()
                            block.append(kvb[l, n, s].reshape(128, 128))
                        else:
                            for j in range(2):
                                keys_in(l, n, k, j).wait_recv()
                            block.append(kvb[l, n, seq_src[k]].reshape(128, 128))
                    kv = jnp.concatenate(block, axis=0)
                    e = jnp.exp(dot_t(q, kv) * scale)
                    den = den + e[:, :128] + e[:, 128:]
                    num = num + dot(e.astype(BF16), kv)
            att = num / jnp.sum(den, axis=-1, keepdims=True)
            for n in range(2):
                for h in range(2):
                    r = 128 * h + 64 * n
                    ax[h, n] = jnp.where(
                        left64[:32], pltpu.roll(att[r : r + 32], 64, 1), att[r + 32 : r + 64]
                    ).astype(BF16)
                for k in range(7):
                    for j in range(2):
                        mixed_out(n, k, j).start()
                partner(ax.at[1 - i, n], ab.at[n, v], 2 + n).start()
                ab[n, v] = ax[i, n]
            for n in range(2):
                for k in range(7):
                    for h in range(2):
                        keys_out(l, n, k, h).wait_send()
                partner(kvo.at[1 - i, n], kvb.at[l, n, s, i], 5 + n).wait_send()
            partner(qx.at[1 - i], qb.at[i], 1).wait_send()

            @pl.when(step == 0)
            def _():
                wo_pass(l, 1 - i).wait_recv()
                wo_pass(l, i).wait_send()
                for k in range(7):
                    wo_copy(l, k).wait_send()
                for dz in (1, 2, 3):
                    wo_quarter(l, dz, False).wait_send()

            for n in range(2):
                partner(ax.at[1 - i, n], ab.at[n, p * 2 + 1 - i], 2 + n).wait_recv()
                for k in range(7):
                    for j in range(2):
                        mixed_in(n, k, j).wait_recv()
                for q in range(8):
                    even, odd = ab[n, 2 * q].astype(F32), ab[n, 2 * q + 1].astype(F32)
                    cols = pl.ds(q * 128, 128)
                    at[n, pl.ds(0, 32), cols] = jnp.where(left64[:32], even, pltpu.roll(odd, 64, 1)).astype(BF16)
                    at[n, pl.ds(32, 32), cols] = jnp.where(left64[:32], pltpu.roll(even, 64, 1), odd).astype(BF16)
                rows = xg[n].astype(F32).reshape(64, 1024) + dot(at[n], wo[l].reshape(1024, 1024))
                rs[n] = rows.reshape(8, 8, 1024)
                x = layer_norm(rows, gains[l, pl.ds(1, 1), :]).astype(BF16)
                part = jnp.zeros((64, 1024), F32)
                for h in range(2):
                    hid = dot(x, wu[h, l])
                    hid = 0.5 * hid * (1.0 + lax.erf(hid * (0.5 ** 0.5)))
                    part = part + dot(hid.astype(BF16), wd[h, l])
                pb[n] = part.reshape(8, 8, 1024).astype(BF16)
                for k in range(7):
                    sums(n, k).start()

            @pl.when((step == 0) & (l == 0))
            def _():
                wo_spread(1)

            for n in range(2):
                own = rs[n, p] + pb[n, p].astype(F32)
                for k in (6, 5, 4, 3, 2, 1, 0):
                    sums(n, k).wait_recv()
                    own = own + rsb[n, k].astype(F32)

                @pl.when(l < LAYERS - 1)
                def _(n=n, own=own):
                    start_gather(n, own)

                resid[pl.ds(8 * n, 8), :] = own
            for n in range(2):
                for k in range(7):
                    sums(n, k).wait_send()
                    for j in range(2):
                        mixed_out(n, k, j).wait_send()
                partner(ax.at[1 - i, n], ab.at[n, v], 2 + n).wait_send()
            return carry

        lax.fori_loop(0, LAYERS, layer_body, 0)
        fb[i] = layer_norm(resid[...], fgain[...]).astype(BF16)
        c = partner(fb.at[i], fb.at[i], 4)
        c.start()
        partner(fb.at[i], fb.at[1 - i], 4).wait_recv()
        fin = fb[...].reshape(32, 1024)
        for q in range(8):
            d = dot_t(fin, headp[q])
            st[q] = st[q] + d
            db[step, q] = d.astype(BF16)
        c.wait_send()
        for k in range(7):
            remote(db.at[step, var_dst[k]], dlr.at[step, p], s_d_s.at[step, k], s_d_r.at[step, k],
                   var_dev(var_dst[k])).start()
        dlr[step, p] = db[step, p]
        return carry

    lax.fori_loop(0, STEPS, step_body, 0)

    state = fields[:, 0, :]
    for step in range(STEPS):
        for k in range(7):
            c = remote(db.at[step, var_dst[k]], dlr.at[step, var_src[k]], s_d_s.at[step, k],
                       s_d_r.at[step, k], var_dev(var_dst[k]))
            c.wait_recv()
            c.wait_send()
        d = jnp.transpose(dlr[step].astype(F32).reshape(256, 128))
        state = state + d[:48]
        out[step] = state.reshape(48, 1, 256)


def per_device(
    fields, channel_ids, lead_index, embed_weight, var_table, agg_query, agg_kv, agg_out,
    agg_temp, pos_table, lead_table, norm_gain, qkv_weight, attn_temp, out_weight,
    up_weight, down_weight, final_gain, head_weight,
):
    vm = pl.BlockSpec(memory_space=pltpu.VMEM)
    sm = pl.BlockSpec(memory_space=pltpu.SMEM)
    hb = pl.BlockSpec(memory_space=pl.ANY)
    dma = pltpu.SemaphoreType.DMA
    V = pltpu.VMEM
    qkv_t = jnp.transpose(qkv_weight, (0, 2, 3, 1)).reshape(LAYERS, 192, 1024)
    head_t = jnp.transpose(head_weight, (1, 2, 0)).reshape(8, 2, 48, 1024)
    out = pl.pallas_call(
        kernel,
        out_shape=jax.ShapeDtypeStruct((STEPS, 48, 1, 256), F32),
        in_specs=[sm] * 3 + [hb] * 16,
        out_specs=vm,
        scratch_shapes=[
            V((48, 1, 256), F32),
            V((48, 1024), BF16),
            V((16, 64), BF16),
            V((1, 16), F32),
            V((16, 1024), BF16),
            V((LAYERS, 2, 1024), F32),
            V((1, 1024), F32),
            V((1024, 2, 1024), BF16),
            V((LAYERS, 2, 128, 1024), BF16),
            V((LAYERS, 2, 128, 1024), BF16),
            V((LAYERS, 8, 2, 64, 1024), BF16),
            V((2, LAYERS, 1024, 256), BF16),
            V((2, LAYERS, 256, 1024), BF16),
            V((1024, 2048), BF16),
            V((1024, 1024), BF16),
            V((8, 128, 1024), BF16),
            V((16, 1024), BF16),
            V((8, 32, 128), F32),
            V((8, 32, 128), F32),
            V((8, 48, 1024), BF16),
            V((8, 64, 2048), BF16),
            V((8, 96, 1024), BF16),
            V((8, 96, 1024), BF16),
            V((8, 96, 1024), BF16),
            V((8, 96, 128), BF16),
            V((2, 16, 2048), F32),
            V((16, 2048), F32),
            V((128, 1024), BF16),
            V((128, 1024), BF16),
            V((16, 1024), F32),
            V((2, 8, 8, 1024), BF16),
            V((2, 8, 8, 1024), BF16),
            V((2, 7, 8, 1024), BF16),
            V((2, 2, 64, 128), BF16),
            V((2, 2, 64, 128), BF16),
            V((LAYERS, 2, 8, 2, 64, 128), BF16),
            V((2, 2, 64, 128), BF16),
            V((2, 2, 32, 128), BF16),
            V((2, 16, 32, 128), BF16),
            V((2, 64, 1024), BF16),
            V((2, 8, 8, 1024), F32),
            V((2, 16, 1024), BF16),
            V((STEPS, 8, 32, 128), BF16),
            V((STEPS, 8, 32, 128), BF16),
            dma((17,)),
            dma((5,)), dma((5,)),
            dma((7,)), dma((7,)),
            dma((7,)), dma((7,)),
            dma((2, 7)), dma((2, 7)),
            dma((2, 7)), dma((2, 7)),
            dma((2, 14)), dma((LAYERS, 2, 14)),
            dma((7,)), dma((7,)),
            dma((STEPS, 7)), dma((STEPS, 7)),
            dma((2, 14)), dma((2, 14)),
            dma((LAYERS, 7)), dma((LAYERS, 7)),
            dma((LAYERS, 3)), dma((LAYERS, 3)),
            dma((LAYERS,)), dma((LAYERS,)),
        ],
        compiler_params=pltpu.CompilerParams(
            collective_id=0, has_side_effects=True, vmem_limit_bytes=60 * 1024 * 1024
        ),
        name="rollout",
    )(
        channel_ids,
        lead_index,
        attn_temp.reshape(LAYERS),
        fields.reshape(48, 1, 256),
        embed_weight.reshape(48, 1024),
        var_table,
        agg_query,
        agg_kv,
        agg_out,
        agg_temp.reshape(1, 16),
        pos_table,
        lead_table,
        norm_gain,
        qkv_t,
        out_weight.reshape(LAYERS, 64, 1024),
        up_weight,
        down_weight,
        final_gain.reshape(1, 1024),
        head_t,
    )
    return out.reshape(STEPS, 3, 16, 1, 256)


def solution(mesh):
    return jax.shard_map(
        per_device,
        mesh=mesh,
        in_specs=(
            P("var", None, None, "seq"),
            P("var"),
            P(),
            P("var", None, None),
            P(),
            P(),
            P(),
            P(),
            P(),
            P("seq", None),
            P(),
            P(),
            P(None, None, "var", None),
            P(None, "var"),
            P(None, "var", None, None),
            P(None, None, "var"),
            P(None, "var", None),
            P(),
            P(),
        ),
        out_specs=P(None, "var", None, None, "seq"),
        check_vma=False,
    )
```

```python
import jax
import jax.numpy as jnp
from jax import lax
from jax.experimental import pallas as pl
from jax.experimental.pallas import tpu as pltpu
from jax.sharding import PartitionSpec as P

STEPS = 2
LAYERS = 2
EPS_NORM = 1e-05
EPS_UNIT = 1e-06
F32 = jnp.float32
BF16 = jnp.bfloat16
MESH = pl.DeviceIdType.MESH

VAR_OFFS = ((2, 1), (1, 1), (3, 1), (2, 0), (0, 1), (1, 0), (3, 0))
SEQ_OFFS = ((2, 1), (1, 1), (3, 1), (0, 1), (2, 0), (1, 0), (3, 0))


def dot(a, b):
    return lax.dot_general(a, b, (((1,), (0,)), ((), ())), preferred_element_type=F32)


def dot_t(a, b):
    return lax.dot_general(a, b, (((1,), (1,)), ((), ())), preferred_element_type=F32)


def layer_norm(values, gain):
    centre = values - jnp.mean(values, axis=-1, keepdims=True)
    spread = jnp.mean(centre * centre, axis=-1, keepdims=True)
    return centre * lax.rsqrt(spread + EPS_NORM) * gain


def kernel(
    ids_h, lead_h, temp_h, fields_h, emb, vart_h, aquery_h, kv_h, aout_h, atemp_h, pos_h, leadt_h, gains_h,
    qkv_h, wo_h, up_h, dn_h, fgain_h, head_h,
    out,
    ids, lead, temp, fields, vart, aquery, atemp, leadt, gains, fgain, kv3,
    wq, wkv, wo, wu, wd, kvv, aout, headp, posv,
    fsnd, st, we, mb, m0, n0, p0r, p0x, p0b, kb, k2, vv, wb, ndx, ndr, hexp, qexp,
    resid, xg, pb, rsb, qb, qx, kvb, kvo, ax, ab, at, rs, fb, db, dlr,
    s_loc, s_sc, s_ws, s_wr, s_is, s_ir, s_es, s_er, s_ag_s, s_ag_r, s_rs_s, s_rs_r,
    s_kv_s, s_kv_r, s_px_s, s_px_r, s_d_s, s_d_r,
    s_at_s, s_at_r, s_wo_s, s_wo_r, s_wz_s, s_wz_r, s_wp_s, s_wp_r, s_p0_s, s_p0_r,
):
    s = lax.axis_index("seq")
    v = lax.axis_index("var")
    i = v % 2
    p = v // 2
    px = p % 4
    py = p // 4
    sz = s // 2
    sy = s % 2
    other = (s, p * 2 + (1 - i))

    var_dst = []
    var_src = []
    for dx, dy in VAR_OFFS:
        var_dst.append(((py + dy) % 2) * 4 + (px + dx) % 4)
        var_src.append(((py + 2 - dy) % 2) * 4 + (px + 4 - dx) % 4)
    seq_dst = []
    seq_src = []
    for dz, dy in SEQ_OFFS:
        seq_dst.append(((sz + dz) % 4) * 2 + (sy + dy) % 2)
        seq_src.append(((sz + 4 - dz) % 4) * 2 + (sy + 2 - dy) % 2)

    def var_dev(q):
        return (s, q * 2 + i)

    def remote(src, dst, send, recv, dev):
        return pltpu.make_async_remote_copy(
            src_ref=src, dst_ref=dst, send_sem=send, recv_sem=recv, device_id=dev, device_id_type=MESH
        )

    own_heads = ((qkv_h.at[:, pl.ds(0, 64)], wq.at[:, i, pl.ds(0, 64)]),
                 (qkv_h.at[:, pl.ds(64, 128)], wkv.at[:, i]),
                 (up_h, wu.at[i]),
                 (dn_h, wd.at[i]))
    mine = pl.ds(sz * 16, 16)
    loads = []
    for k, (a, b) in enumerate((
        (fields_h, fields), (kv_h, kv3), (emb, we.at[p]), (aquery_h, aquery), (vart_h, vart), (atemp_h, atemp),
        (aout_h, aout), (pos_h.at[pl.ds(v * 16, 16)], posv), (leadt_h, leadt), (gains_h, gains),
        (fgain_h, fgain), (head_h.at[:, i], headp.at[:, pl.ds(0, 48)]), *own_heads, (wo_h.at[:, mine], wo.at[:, p, i, mine]),
    )):
        loads.append(pltpu.make_async_copy(a, b, s_loc.at[k]))
    scalars = [pltpu.make_async_copy(a, b, s_sc.at[k])
               for k, (a, b) in enumerate(((ids_h, ids), (lead_h, lead), (temp_h, temp)))]
    for c in (*scalars, *loads[:6]):
        c.start()

    bar = pltpu.get_barrier_semaphore()
    for q in var_dst:
        for j in range(2):
            pl.semaphore_signal(bar, inc=1, device_id=(s, q * 2 + j), device_id_type=MESH)
    for t in seq_dst:
        for j in range(2):
            pl.semaphore_signal(bar, inc=1, device_id=(t, p * 2 + j), device_id_type=MESH)
    pl.semaphore_signal(bar, inc=1, device_id=other, device_id_type=MESH)

    for c in loads[6:]:
        c.start()
    scalars[0].wait()
    loads[0].wait()
    state0 = fields[:, 0, :]
    frow = lax.broadcasted_iota(jnp.int32, (80, 256), 0)
    fcol = lax.broadcasted_iota(jnp.int32, (80, 256), 1) % 32
    named = jnp.where(fcol == 0, ids[0], jnp.where(fcol == 1, ids[1], jnp.where(fcol == 2, ids[2], 0)))
    extra = jnp.where(frow == 0, named, 0).astype(F32)
    fsnd[...] = jnp.transpose(jnp.concatenate([state0, extra], axis=0)).reshape(8, 32, 128)

    def emb_copy(k, src):
        return remote(emb, we.at[src], s_es.at[k], s_er.at[k], var_dev(var_dst[k]))

    def field_copy(k, src):
        return remote(fsnd.at[var_dst[k]], st.at[src], s_is.at[k], s_ir.at[k], var_dev(var_dst[k]))

    wcopies = []
    for k, (a, b) in enumerate(own_heads):
        wcopies.append(remote(a, b, s_ws.at[k], s_wr.at[k], other))

    def wo_copy(l, k):
        return remote(wo_h.at[l, mine], wo.at[l, p, i, mine], s_wo_s.at[l, k], s_wo_r.at[l, k], var_dev(var_dst[k]))

    def wo_arrival(l, k):
        return remote(wo_h.at[l, mine], wo.at[l, var_src[k], i, mine], s_wo_s.at[l, k], s_wo_r.at[l, k],
                      var_dev(var_dst[k]))

    def wo_quarter(l, dz, back):
        rows = pl.ds(((sz + 4 - dz) % 4) * 16, 16) if back else mine
        quarter = wo.at[l, :, i, rows]
        return remote(quarter, quarter, s_wz_s.at[l, dz - 1], s_wz_r.at[l, dz - 1], (((sz + dz) % 4) * 2 + sy, v))

    def wo_pass(l, core):
        return remote(wo.at[l, :, core], wo.at[l, :, core], s_wp_s.at[l], s_wp_r.at[l], other)

    def wo_spread(l):
        for k in range(7):
            wo_arrival(l, k).wait_recv()
        for dz in (2, 1, 3):
            wo_quarter(l, dz, False).start()


    pl.semaphore_wait(bar, 29)
    for c in wcopies:
        c.start()
    for k in range(7):
        wo_copy(0, k).start()
    emb_copy(0, p).start()

    st[p] = fsnd[p]
    wq[:, :, pl.ds(64, 64)] = jnp.zeros((LAYERS, 2, 64, 1024), BF16)
    headp[:, pl.ds(48, 80)] = jnp.zeros((8, 80, 1024), BF16)

    hrow = lax.broadcasted_iota(jnp.int32, (128, 1024), 0)
    hcol = lax.broadcasted_iota(jnp.int32, (128, 1024), 1) // 64
    hexp[...] = jnp.where(hrow == hcol, 1.0, 0.0).astype(BF16)
    loads[3].wait()
    aq = aquery[...].astype(F32)
    aq = aq * lax.rsqrt(jnp.mean(aq * aq, axis=-1, keepdims=True) + EPS_UNIT)
    aqt = jnp.concatenate([aq] * 16, axis=1)
    aqt = jnp.concatenate([aqt, jnp.zeros((112, 1024), F32)], axis=0)
    qexp[...] = jnp.where(hrow == hcol, aqt, 0.0).astype(BF16)
    for c in loads[4:6]:
        c.wait()
    tvec = jnp.concatenate([atemp[...] * (1.0 / 64.0), jnp.zeros((1, 112), F32)], axis=1)

    loads[1].wait()

    def split_kv(n, c):
        rows = pl.ds(n * 64, 64)
        kvv[rows] = kv3[rows].reshape(64, 2048)
        return c

    lax.fori_loop(0, 16, split_kv, 0)
    loads[2].wait()
    hrow16 = lax.broadcasted_iota(jnp.int32, (16, 48), 0)
    hcol16 = lax.broadcasted_iota(jnp.int32, (16, 48), 1)
    idv = jnp.where(hrow16 == 0, ids[0], jnp.where(hrow16 == 1, ids[1], ids[2]))
    hot = jnp.where((idv == hcol16) & (hrow16 < 3), 1.0, 0.0).astype(BF16)
    lhs = jnp.concatenate([we[p], dot(hot, vart[...]).astype(BF16)], axis=0)
    for n in range(4):
        cols = pl.ds(n * 512, 512)
        m0[:, cols] = dot(lhs, kvv[:, cols]).astype(BF16)

    def all_channels():
        for k in range(7):
            field_copy(k, var_src[k]).wait_recv()
        nrow = lax.broadcasted_iota(jnp.int32, (128, 48), 0) % 16
        ncol = lax.broadcasted_iota(jnp.int32, (128, 48), 1).astype(F32)
        named = st[:, pl.ds(0, 16)].reshape(128, 128)[:, 48:49]
        hot = jnp.where((named == ncol) & (nrow < 3), 1.0, 0.0).astype(BF16)
        vall = dot(hot, vart[...]).astype(BF16)
        for n in range(4):
            cols = pl.ds(n * 512, 512)
            mb[:, pl.ds(48, 16), cols] = dot(vall, kvv[:, cols]).astype(BF16).reshape(8, 16, 512)
        for k in range(7):
            emb_copy(k, var_src[k]).wait_recv()
        wall = we[...].reshape(384, 1024)
        for n in range(4):
            cols = pl.ds(n * 512, 512)
            mb[:, pl.ds(0, 48), cols] = dot(wall, kvv[:, cols]).astype(BF16).reshape(8, 48, 512)
        for k in range(7):
            field_copy(k, p).wait_send()
            emb_copy(k, p).wait_send()

    lane64 = lax.broadcasted_iota(jnp.int32, (32, 64), 1)
    left64 = lax.broadcasted_iota(jnp.int32, (64, 128), 1) < 64

    def partner(src, dst, k):
        return remote(src, dst, s_px_s.at[k], s_px_r.at[k], other)

    def gather(c, k, src):
        return remote(xg.at[c, p], xg.at[c, src], s_ag_s.at[c, k], s_ag_r.at[c, k], var_dev(var_dst[k]))

    def start_gather(c, own):
        xg[c, p] = own.astype(BF16)
        for k in range(7):
            gather(c, k, p).start()

    def sums(c, k):
        return remote(pb.at[c, var_dst[k]], rsb.at[c, k], s_rs_s.at[c, k], s_rs_r.at[c, k], var_dev(var_dst[k]))

    def keys_out(l, c, k, h):
        return remote(kvo.at[h, c], kvb.at[l, c, s, i], s_kv_s.at[c, 2 * k + h], s_kv_r.at[l, c, 2 * k + i],
                      (seq_dst[k], p * 2 + h))

    def keys_in(l, c, k, j):
        return remote(kvo.at[j, c], kvb.at[l, c, seq_src[k], j], s_kv_s.at[c, 2 * k + j],
                      s_kv_r.at[l, c, 2 * k + j], (seq_dst[k], p * 2 + j))

    def mixed_out(c, k, j):
        return remote(ax.at[j, c], ab.at[c, v], s_at_s.at[c, 2 * k + j], s_at_r.at[c, 2 * k + i],
                      (s, var_dst[k] * 2 + j))

    def mixed_in(c, k, j):
        return remote(ax.at[j, c], ab.at[c, var_src[k] * 2 + j], s_at_s.at[c, 2 * k + j], s_at_r.at[c, 2 * k + j],
                      (s, var_dst[k] * 2 + j))

    def pool_products(blocks, mat):
        for q in range(8):
            sb = blocks[q][:, :64]
            blk = jnp.concatenate(
                [jnp.where(lane64 // 16 == n, sb, jnp.where(lane64 == 48 + n, 1.0, 0.0)) for n in range(3)], axis=0
            ).astype(BF16)
            kk = dot(blk, mat(q, pl.ds(0, 1024)))
            kb[q] = kk.astype(BF16)
            k2[q] = (kk * kk).astype(BF16)
            vv[q] = dot(blk, mat(q, pl.ds(1024, 1024))).astype(BF16)
        ss = dot_t(k2[...].reshape(768, 1024), hexp[...])
        qk = dot_t(kb[...].reshape(768, 1024), qexp[...])
        w = jnp.exp(qk * lax.rsqrt(ss * (1.0 / 64.0) + EPS_UNIT) * tvec)
        wb[...] = w.astype(BF16).reshape(8, 96, 128)

    def start_rows(pooled, step):
        row16 = lax.broadcasted_iota(jnp.int32, (16, 16), 1)
        lhot = jnp.where(row16 == lead[0] + step, 1.0, 0.0).astype(BF16)
        add = posv[...].astype(F32) + dot(lhot, leadt[...])
        own = dot(pooled.astype(BF16), aout[...]) + add
        for n in range(2):
            start_gather(n, own[8 * n : 8 * n + 8])

    pool_products(fsnd, lambda q, cols: m0[:, cols])
    for q in range(8):
        wx = dot(wb[q], hexp[...])
        nx = wx * vv[q].astype(F32)
        wq3 = wb[q].astype(F32)
        n0[:, q, :, pl.ds(0, 1024)] = (nx[0:32] + nx[32:64] + nx[64:96]).reshape(2, 16, 1024).astype(BF16)
        n0[:, q, :, pl.ds(1024, 128)] = (wq3[0:32] + wq3[32:64] + wq3[64:96]).reshape(2, 16, 128).astype(BF16)
    c0 = partner(n0.at[1 - i], p0r, 7)
    c0.start()
    for c in loads[6:12]:
        c.wait()
    loads[16].wait()
    c0.wait_recv()
    p0x[...] = (n0[i].astype(F32) + p0r[...].astype(F32)).astype(BF16)

    def pool_sums(k):
        return remote(p0x.at[var_dst[k]], p0b.at[k], s_p0_s.at[k], s_p0_r.at[k], var_dev(var_dst[k]))

    for k in range(7):
        pool_sums(k).start()
    wo_spread(0)
    for c in scalars[1:]:
        c.wait()
    tot = p0x[p].astype(F32)
    for k in (6, 5, 4, 3, 2, 1, 0):
        pool_sums(k).wait_recv()
        tot = tot + p0b[k].astype(F32)
    inv = 1.0 / tot[:, 1024:]
    inv_hi = inv.astype(BF16)
    inv_lo = (inv - inv_hi.astype(F32)).astype(BF16)
    start_rows(tot[:, :1024] * (dot(inv_hi, hexp[...]) + dot(inv_lo, hexp[...])), 0)
    c0.wait_send()
    for k in range(7):
        pool_sums(k).wait_send()
    for c in loads[12:16]:
        c.wait()
    for c in wcopies:
        c.wait()

    def step_body(step, carry):
        @pl.when(step == 1)
        def _():
            pool_products(st, lambda q, cols: mb[q, :, cols])
            num = jnp.zeros((32, 1024), F32)
            den = jnp.zeros((32, 1024), F32)
            for q in range(8):
                wx = dot(wb[q], hexp[...])
                nx = wx * vv[q].astype(F32)
                num = num + (nx[0:32] + nx[32:64] + nx[64:96])
                den = den + (wx[0:32] + wx[32:64] + wx[64:96])
            ndx[:, :, pl.ds(0, 1024)] = num.reshape(2, 16, 1024)
            ndx[:, :, pl.ds(1024, 1024)] = den.reshape(2, 16, 1024)
            c = partner(ndx.at[1 - i], ndr, 0)
            c.start()
            c.wait_recv()
            tot = ndx[i] + ndr[...]
            start_rows(tot[:, :1024] / tot[:, 1024:], 1)
            c.wait_send()

        def layer_body(l, carry):
            for n in range(2):
                for k in range(7):
                    gather(n, k, var_src[k]).wait_recv()
                x = layer_norm(xg[n].astype(F32).reshape(64, 1024), gains[l, pl.ds(0, 1), :]).astype(BF16)
                both = dot_t(x, wkv[l].reshape(256, 1024))
                for h in range(2):
                    kv = both[:, 128 * h : 128 * h + 128]
                    kq = jnp.where(left64, kv * kv, 0.0)
                    scale = lax.rsqrt(jnp.sum(kq, axis=-1, keepdims=True) * (1.0 / 64.0) + EPS_UNIT)
                    kvo[h, n] = (kv * jnp.where(left64, scale, 1.0)).astype(BF16)
                for k in range(7):
                    for h in range(2):
                        keys_out(l, n, k, h).start()
                partner(kvo.at[1 - i, n], kvb.at[l, n, s, i], 5 + n).start()
                kvb[l, n, s, i] = kvo[i, n]
                both = dot_t(x, wq[l].reshape(256, 1024))
                for h in range(2):
                    q = both[:, 128 * h : 128 * h + 128]
                    q = q * lax.rsqrt(jnp.sum(q * q, axis=-1, keepdims=True) * (1.0 / 64.0) + EPS_UNIT)
                    qx[h, n] = q.astype(BF16)
            partner(qx.at[1 - i], qb.at[i], 1).start()
            qb[i] = qx[i]

            @pl.when((step == 0) & (l == 0))
            def _():
                for k in range(7):
                    wo_copy(1, k).start()
                for k in (1, 2, 3):
                    emb_copy(k, p).start()

            @pl.when((step == 0) & (l == 1))
            def _():
                for k in (4, 5, 6):
                    emb_copy(k, p).start()
                for k in range(7):
                    field_copy(k, p).start()

            @pl.when(step == 0)
            def _():
                for dz in (1, 2, 3):
                    wo_quarter(l, dz, True).wait_recv()
                wo_pass(l, i).start()

            for n in range(2):
                for k in range(7):
                    gather(n, k, p).wait_send()
            partner(qx.at[1 - i], qb.at[1 - i], 1).wait_recv()
            scale = temp[l] * (1.0 / 64.0)
            q = qb[...].reshape(256, 128)
            num = jnp.zeros((256, 128), F32)
            den = jnp.zeros((256, 128), F32)
            for n in range(2):
                for pair in ((7, 6), (5, 4), (3, 2), (1, 0)):
                    block = []
                    for k in pair:
                        if k == 7:
                            partner(kvo.at[1 - i, n], kvb.at[l, n, s, 1 - i], 5 + n).wait_recv()
                            block.append(kvb[l, n, s].reshape(128, 128))
                        else:
                            for j in range(2):
                                keys_in(l, n, k, j).wait_recv()
                            block.append(kvb[l, n, seq_src[k]].reshape(128, 128))
                    kv = jnp.concatenate(block, axis=0)
                    e = jnp.exp(dot_t(q, kv) * scale)
                    den = den + e[:, :128] + e[:, 128:]
                    num = num + dot(e.astype(BF16), kv)
            att = num / jnp.sum(den, axis=-1, keepdims=True)
            for n in range(2):
                for h in range(2):
                    r = 128 * h + 64 * n
                    ax[h, n] = jnp.where(
                        left64[:32], pltpu.roll(att[r : r + 32], 64, 1), att[r + 32 : r + 64]
                    ).astype(BF16)
                for k in range(7):
                    for j in range(2):
                        mixed_out(n, k, j).start()
                partner(ax.at[1 - i, n], ab.at[n, v], 2 + n).start()
                ab[n, v] = ax[i, n]
            for n in range(2):
                for k in range(7):
                    for h in range(2):
                        keys_out(l, n, k, h).wait_send()
                partner(kvo.at[1 - i, n], kvb.at[l, n, s, i], 5 + n).wait_send()
            partner(qx.at[1 - i], qb.at[i], 1).wait_send()

            @pl.when(step == 0)
            def _():
                wo_pass(l, 1 - i).wait_recv()
                wo_pass(l, i).wait_send()
                for k in range(7):
                    wo_copy(l, k).wait_send()
                for dz in (1, 2, 3):
                    wo_quarter(l, dz, False).wait_send()

            @pl.when((step == 0) & (l == 1))
            def _():
                all_channels()

            for n in range(2):
                partner(ax.at[1 - i, n], ab.at[n, p * 2 + 1 - i], 2 + n).wait_recv()
                for k in range(7):
                    for j in range(2):
                        mixed_in(n, k, j).wait_recv()
                for q in range(8):
                    even, odd = ab[n, 2 * q].astype(F32), ab[n, 2 * q + 1].astype(F32)
                    cols = pl.ds(q * 128, 128)
                    at[n, pl.ds(0, 32), cols] = jnp.where(left64[:32], even, pltpu.roll(odd, 64, 1)).astype(BF16)
                    at[n, pl.ds(32, 32), cols] = jnp.where(left64[:32], pltpu.roll(even, 64, 1), odd).astype(BF16)
                rows = xg[n].astype(F32).reshape(64, 1024) + dot(at[n], wo[l].reshape(1024, 1024))
                rs[n] = rows.reshape(8, 8, 1024)
                x = layer_norm(rows, gains[l, pl.ds(1, 1), :]).astype(BF16)
                part = jnp.zeros((64, 1024), F32)
                for h in range(2):
                    hid = dot(x, wu[h, l])
                    hid = 0.5 * hid * (1.0 + lax.erf(hid * (0.5 ** 0.5)))
                    part = part + dot(hid.astype(BF16), wd[h, l])
                pb[n] = part.reshape(8, 8, 1024).astype(BF16)
                for k in range(7):
                    sums(n, k).start()

            @pl.when((step == 0) & (l == 0))
            def _():
                wo_spread(1)

            for n in range(2):
                own = rs[n, p] + pb[n, p].astype(F32)
                for k in (6, 5, 4, 3, 2, 1, 0):
                    sums(n, k).wait_recv()
                    own = own + rsb[n, k].astype(F32)

                @pl.when(l < LAYERS - 1)
                def _(n=n, own=own):
                    start_gather(n, own)

                resid[pl.ds(8 * n, 8), :] = own
            for n in range(2):
                for k in range(7):
                    sums(n, k).wait_send()
                    for j in range(2):
                        mixed_out(n, k, j).wait_send()
                partner(ax.at[1 - i, n], ab.at[n, v], 2 + n).wait_send()
            return carry

        lax.fori_loop(0, LAYERS, layer_body, 0)
        fb[i] = layer_norm(resid[...], fgain[...]).astype(BF16)
        c = partner(fb.at[i], fb.at[i], 4)
        c.start()
        partner(fb.at[i], fb.at[1 - i], 4).wait_recv()
        fin = fb[...].reshape(32, 1024)
        for q in range(8):
            d = dot_t(fin, headp[q])
            st[q] = st[q] + d
            db[step, q] = d.astype(BF16)
        c.wait_send()
        for k in range(7):
            remote(db.at[step, var_dst[k]], dlr.at[step, p], s_d_s.at[step, k], s_d_r.at[step, k],
                   var_dev(var_dst[k])).start()
        dlr[step, p] = db[step, p]
        return carry

    lax.fori_loop(0, STEPS, step_body, 0)

    state = fields[:, 0, :]
    for step in range(STEPS):
        for k in range(7):
            c = remote(db.at[step, var_dst[k]], dlr.at[step, var_src[k]], s_d_s.at[step, k],
                       s_d_r.at[step, k], var_dev(var_dst[k]))
            c.wait_recv()
            c.wait_send()
        d = jnp.transpose(dlr[step].astype(F32).reshape(256, 128))
        state = state + d[:48]
        out[step] = state.reshape(48, 1, 256)


def per_device(
    fields, channel_ids, lead_index, embed_weight, var_table, agg_query, agg_kv, agg_out,
    agg_temp, pos_table, lead_table, norm_gain, qkv_weight, attn_temp, out_weight,
    up_weight, down_weight, final_gain, head_weight,
):
    vm = pl.BlockSpec(memory_space=pltpu.VMEM)
    hb = pl.BlockSpec(memory_space=pl.ANY)
    dma = pltpu.SemaphoreType.DMA
    V = pltpu.VMEM
    qkv_t = jnp.transpose(qkv_weight, (0, 2, 3, 1)).reshape(LAYERS, 192, 1024)
    head_t = jnp.transpose(head_weight, (1, 2, 0)).reshape(8, 2, 48, 1024)
    out = pl.pallas_call(
        kernel,
        out_shape=jax.ShapeDtypeStruct((STEPS, 48, 1, 256), F32),
        in_specs=[hb] * 19,
        out_specs=vm,
        scratch_shapes=[
            pltpu.SMEM((3,), jnp.int32),
            pltpu.SMEM((1,), jnp.int32),
            pltpu.SMEM((LAYERS,), F32),
            V((48, 1, 256), F32),
            V((48, 1024), BF16),
            V((16, 64), BF16),
            V((1, 16), F32),
            V((16, 1024), BF16),
            V((LAYERS, 2, 1024), F32),
            V((1, 1024), F32),
            V((1024, 2, 1024), BF16),
            V((LAYERS, 2, 128, 1024), BF16),
            V((LAYERS, 2, 128, 1024), BF16),
            V((LAYERS, 8, 2, 64, 1024), BF16),
            V((2, LAYERS, 1024, 256), BF16),
            V((2, LAYERS, 256, 1024), BF16),
            V((1024, 2048), BF16),
            V((1024, 1024), BF16),
            V((8, 128, 1024), BF16),
            V((16, 1024), BF16),
            V((8, 32, 128), F32),
            V((8, 32, 128), F32),
            V((8, 48, 1024), BF16),
            V((8, 64, 2048), BF16),
            V((64, 2048), BF16),
            V((2, 8, 16, 1152), BF16),
            V((8, 16, 1152), BF16),
            V((8, 16, 1152), BF16),
            V((7, 16, 1152), BF16),
            V((8, 96, 1024), BF16),
            V((8, 96, 1024), BF16),
            V((8, 96, 1024), BF16),
            V((8, 96, 128), BF16),
            V((2, 16, 2048), F32),
            V((16, 2048), F32),
            V((128, 1024), BF16),
            V((128, 1024), BF16),
            V((16, 1024), F32),
            V((2, 8, 8, 1024), BF16),
            V((2, 8, 8, 1024), BF16),
            V((2, 7, 8, 1024), BF16),
            V((2, 2, 64, 128), BF16),
            V((2, 2, 64, 128), BF16),
            V((LAYERS, 2, 8, 2, 64, 128), BF16),
            V((2, 2, 64, 128), BF16),
            V((2, 2, 32, 128), BF16),
            V((2, 16, 32, 128), BF16),
            V((2, 64, 1024), BF16),
            V((2, 8, 8, 1024), F32),
            V((2, 16, 1024), BF16),
            V((STEPS, 8, 32, 128), BF16),
            V((STEPS, 8, 32, 128), BF16),
            dma((17,)),
            dma((3,)),
            dma((5,)), dma((5,)),
            dma((7,)), dma((7,)),
            dma((7,)), dma((7,)),
            dma((2, 7)), dma((2, 7)),
            dma((2, 7)), dma((2, 7)),
            dma((2, 14)), dma((LAYERS, 2, 14)),
            dma((8,)), dma((8,)),
            dma((STEPS, 7)), dma((STEPS, 7)),
            dma((2, 14)), dma((2, 14)),
            dma((LAYERS, 7)), dma((LAYERS, 7)),
            dma((LAYERS, 3)), dma((LAYERS, 3)),
            dma((LAYERS,)), dma((LAYERS,)),
            dma((7,)), dma((7,)),
        ],
        compiler_params=pltpu.CompilerParams(
            collective_id=0, has_side_effects=True, vmem_limit_bytes=60 * 1024 * 1024
        ),
        name="rollout",
    )(
        channel_ids,
        lead_index,
        attn_temp.reshape(LAYERS),
        fields.reshape(48, 1, 256),
        embed_weight.reshape(48, 1024),
        var_table,
        agg_query,
        agg_kv,
        agg_out,
        agg_temp.reshape(1, 16),
        pos_table,
        lead_table,
        norm_gain,
        qkv_t,
        out_weight.reshape(LAYERS, 64, 1024),
        up_weight,
        down_weight,
        final_gain.reshape(1, 1024),
        head_t,
    )
    return out.reshape(STEPS, 3, 16, 1, 256)


def solution(mesh):
    return jax.shard_map(
        per_device,
        mesh=mesh,
        in_specs=(
            P("var", None, None, "seq"),
            P("var"),
            P(),
            P("var", None, None),
            P(),
            P(),
            P(),
            P(),
            P(),
            P("seq", None),
            P(),
            P(),
            P(None, None, "var", None),
            P(None, "var"),
            P(None, "var", None, None),
            P(None, None, "var"),
            P(None, "var", None),
            P(),
            P(),
        ),
        out_specs=P(None, "var", None, None, "seq"),
        check_vma=False,
    )
```

```python
import jax
import jax.numpy as jnp
from jax import lax
from jax.experimental import pallas as pl
from jax.experimental.pallas import tpu as pltpu
from jax.sharding import PartitionSpec as P

STEPS = 2
LAYERS = 2
EPS_NORM = 1e-05
EPS_UNIT = 1e-06
F32 = jnp.float32
BF16 = jnp.bfloat16
MESH = pl.DeviceIdType.MESH

VAR_OFFS = ((2, 1), (1, 1), (3, 1), (2, 0), (0, 1), (1, 0), (3, 0))
SEQ_OFFS = ((2, 1), (1, 1), (3, 1), (0, 1), (2, 0), (1, 0), (3, 0))


def dot(a, b):
    return lax.dot_general(a, b, (((1,), (0,)), ((), ())), preferred_element_type=F32)


def dot_t(a, b):
    return lax.dot_general(a, b, (((1,), (1,)), ((), ())), preferred_element_type=F32)


def layer_norm(values, gain):
    centre = values - jnp.mean(values, axis=-1, keepdims=True)
    spread = jnp.mean(centre * centre, axis=-1, keepdims=True)
    return centre * lax.rsqrt(spread + EPS_NORM) * gain


def kernel(
    ids_h, lead_h, temp_h, fields_h, emb, vart_h, aquery_h, kv_h, aout_h, atemp_h, pos_h, leadt_h, gains_h,
    qkv_h, wo_h, up_h, dn_h, fgain_h, head_h,
    out,
    ids, lead, temp, fields, vart, aquery, atemp, leadt, gains, fgain, kv3,
    wq, wkv, wo, wu, wd, kvv, aout, headp, posv,
    fsnd, st, we, mb, m0, n0, p0r, p0x, p0b, kb, k2, vv, wb, ndx, ndr, hexp, qexp,
    resid, xg, pb, rsb, qb, qx, kvb, kvo, ax, ab, at, rs, fb, db, dlr,
    s_loc, s_sc, s_ws, s_wr, s_is, s_ir, s_es, s_er, s_ag_s, s_ag_r, s_rs_s, s_rs_r,
    s_kv_s, s_kv_r, s_px_s, s_px_r, s_d_s, s_d_r,
    s_at_s, s_at_r, s_wo_s, s_wo_r, s_wz_s, s_wz_r, s_wp_s, s_wp_r, s_p0_s, s_p0_r,
):
    s = lax.axis_index("seq")
    v = lax.axis_index("var")
    i = v % 2
    p = v // 2
    px = p % 4
    py = p // 4
    sz = s // 2
    sy = s % 2
    other = (s, p * 2 + (1 - i))

    var_dst = []
    var_src = []
    for dx, dy in VAR_OFFS:
        var_dst.append(((py + dy) % 2) * 4 + (px + dx) % 4)
        var_src.append(((py + 2 - dy) % 2) * 4 + (px + 4 - dx) % 4)
    seq_dst = []
    seq_src = []
    for dz, dy in SEQ_OFFS:
        seq_dst.append(((sz + dz) % 4) * 2 + (sy + dy) % 2)
        seq_src.append(((sz + 4 - dz) % 4) * 2 + (sy + 2 - dy) % 2)

    def var_dev(q):
        return (s, q * 2 + i)

    def remote(src, dst, send, recv, dev):
        return pltpu.make_async_remote_copy(
            src_ref=src, dst_ref=dst, send_sem=send, recv_sem=recv, device_id=dev, device_id_type=MESH
        )

    own_heads = ((qkv_h.at[:, pl.ds(0, 64)], wq.at[:, i, pl.ds(0, 64)]),
                 (qkv_h.at[:, pl.ds(64, 128)], wkv.at[:, i]),
                 (up_h, wu.at[i]),
                 (dn_h, wd.at[i]))
    mine = pl.ds(sz * 16, 16)
    loads = []
    for k, (a, b) in enumerate((
        (fields_h, fields), (kv_h, kv3), (emb, we.at[p]), (aquery_h, aquery), (vart_h, vart), (atemp_h, atemp),
        (aout_h, aout), (pos_h.at[pl.ds(v * 16, 16)], posv), (leadt_h, leadt), (gains_h, gains),
        (fgain_h, fgain), (head_h.at[:, i], headp.at[:, pl.ds(0, 48)]), *own_heads, (wo_h.at[:, mine], wo.at[:, p, i, mine]),
    )):
        loads.append(pltpu.make_async_copy(a, b, s_loc.at[k]))
    scalars = [pltpu.make_async_copy(a, b, s_sc.at[k])
               for k, (a, b) in enumerate(((ids_h, ids), (lead_h, lead), (temp_h, temp)))]
    for c in (*scalars, *loads[:6]):
        c.start()

    bar = pltpu.get_barrier_semaphore()
    for q in var_dst:
        for j in range(2):
            pl.semaphore_signal(bar, inc=1, device_id=(s, q * 2 + j), device_id_type=MESH)
    for t in seq_dst:
        for j in range(2):
            pl.semaphore_signal(bar, inc=1, device_id=(t, p * 2 + j), device_id_type=MESH)
    pl.semaphore_signal(bar, inc=1, device_id=other, device_id_type=MESH)

    for c in loads[6:]:
        c.start()
    scalars[0].wait()
    loads[0].wait()
    state0 = fields[:, 0, :]
    frow = lax.broadcasted_iota(jnp.int32, (80, 256), 0)
    fcol = lax.broadcasted_iota(jnp.int32, (80, 256), 1) % 32
    named = jnp.where(fcol == 0, ids[0], jnp.where(fcol == 1, ids[1], jnp.where(fcol == 2, ids[2], 0)))
    extra = jnp.where(frow == 0, named, 0).astype(F32)
    fsnd[...] = jnp.transpose(jnp.concatenate([state0, extra], axis=0)).reshape(8, 32, 128)

    def emb_copy(k, src):
        return remote(emb, we.at[src], s_es.at[k], s_er.at[k], var_dev(var_dst[k]))

    def field_copy(k, src):
        return remote(fsnd.at[var_dst[k]], st.at[src], s_is.at[k], s_ir.at[k], var_dev(var_dst[k]))

    wcopies = []
    for k, (a, b) in enumerate(own_heads):
        wcopies.append(remote(a, b, s_ws.at[k], s_wr.at[k], other))

    def wo_copy(l, k):
        return remote(wo_h.at[l, mine], wo.at[l, p, i, mine], s_wo_s.at[l, k], s_wo_r.at[l, k], var_dev(var_dst[k]))

    def wo_arrival(l, k):
        return remote(wo_h.at[l, mine], wo.at[l, var_src[k], i, mine], s_wo_s.at[l, k], s_wo_r.at[l, k],
                      var_dev(var_dst[k]))

    def wo_quarter(l, dz, back):
        rows = pl.ds(((sz + 4 - dz) % 4) * 16, 16) if back else mine
        quarter = wo.at[l, :, i, rows]
        return remote(quarter, quarter, s_wz_s.at[l, dz - 1], s_wz_r.at[l, dz - 1], (((sz + dz) % 4) * 2 + sy, v))

    def wo_pass(l, core):
        return remote(wo.at[l, :, core], wo.at[l, :, core], s_wp_s.at[l], s_wp_r.at[l], other)

    def wo_spread(l):
        for k in range(7):
            wo_arrival(l, k).wait_recv()
        for dz in (2, 1, 3):
            wo_quarter(l, dz, False).start()


    pl.semaphore_wait(bar, 29)
    for c in wcopies:
        c.start()
    for l in range(LAYERS):
        for k in range(7):
            wo_copy(l, k).start()

    st[p] = fsnd[p]
    wq[:, :, pl.ds(64, 64)] = jnp.zeros((LAYERS, 2, 64, 1024), BF16)
    headp[:, pl.ds(48, 80)] = jnp.zeros((8, 80, 1024), BF16)

    hrow = lax.broadcasted_iota(jnp.int32, (128, 1024), 0)
    hcol = lax.broadcasted_iota(jnp.int32, (128, 1024), 1) // 64
    hexp[...] = jnp.where(hrow == hcol, 1.0, 0.0).astype(BF16)
    loads[3].wait()
    aq = aquery[...].astype(F32)
    aq = aq * lax.rsqrt(jnp.mean(aq * aq, axis=-1, keepdims=True) + EPS_UNIT)
    aqt = jnp.concatenate([aq] * 16, axis=1)
    aqt = jnp.concatenate([aqt, jnp.zeros((112, 1024), F32)], axis=0)
    qexp[...] = jnp.where(hrow == hcol, aqt, 0.0).astype(BF16)
    for c in loads[4:6]:
        c.wait()
    tvec = jnp.concatenate([atemp[...] * (1.0 / 64.0), jnp.zeros((1, 112), F32)], axis=1)

    loads[1].wait()

    def split_kv(n, c):
        rows = pl.ds(n * 64, 64)
        kvv[rows] = kv3[rows].reshape(64, 2048)
        return c

    lax.fori_loop(0, 16, split_kv, 0)
    loads[2].wait()
    hrow16 = lax.broadcasted_iota(jnp.int32, (16, 48), 0)
    hcol16 = lax.broadcasted_iota(jnp.int32, (16, 48), 1)
    idv = jnp.where(hrow16 == 0, ids[0], jnp.where(hrow16 == 1, ids[1], ids[2]))
    hot = jnp.where((idv == hcol16) & (hrow16 < 3), 1.0, 0.0).astype(BF16)
    lhs = jnp.concatenate([we[p], dot(hot, vart[...]).astype(BF16)], axis=0)
    for n in range(4):
        cols = pl.ds(n * 512, 512)
        m0[:, cols] = dot(lhs, kvv[:, cols]).astype(BF16)

    def all_channels():
        for k in range(7):
            field_copy(k, var_src[k]).wait_recv()
        nrow = lax.broadcasted_iota(jnp.int32, (128, 48), 0) % 16
        ncol = lax.broadcasted_iota(jnp.int32, (128, 48), 1).astype(F32)
        named = st[:, pl.ds(0, 16)].reshape(128, 128)[:, 48:49]
        hot = jnp.where((named == ncol) & (nrow < 3), 1.0, 0.0).astype(BF16)
        vall = dot(hot, vart[...]).astype(BF16)
        for n in range(4):
            cols = pl.ds(n * 512, 512)
            mb[:, pl.ds(48, 16), cols] = dot(vall, kvv[:, cols]).astype(BF16).reshape(8, 16, 512)
        for k in range(7):
            emb_copy(k, var_src[k]).wait_recv()
        wall = we[...].reshape(384, 1024)
        for n in range(4):
            cols = pl.ds(n * 512, 512)
            mb[:, pl.ds(0, 48), cols] = dot(wall, kvv[:, cols]).astype(BF16).reshape(8, 48, 512)
        for k in range(7):
            field_copy(k, p).wait_send()
            emb_copy(k, p).wait_send()

    lane64 = lax.broadcasted_iota(jnp.int32, (32, 64), 1)
    left64 = lax.broadcasted_iota(jnp.int32, (64, 128), 1) < 64

    def partner(src, dst, k):
        return remote(src, dst, s_px_s.at[k], s_px_r.at[k], other)

    def gather(c, k, src):
        return remote(xg.at[c, p], xg.at[c, src], s_ag_s.at[c, k], s_ag_r.at[c, k], var_dev(var_dst[k]))

    def start_gather(c, own):
        xg[c, p] = own.astype(BF16)
        for k in range(7):
            gather(c, k, p).start()

    def sums(c, k):
        return remote(pb.at[c, var_dst[k]], rsb.at[c, k], s_rs_s.at[c, k], s_rs_r.at[c, k], var_dev(var_dst[k]))

    def keys_out(l, c, k, h):
        return remote(kvo.at[h, c], kvb.at[l, c, s, i], s_kv_s.at[c, 2 * k + h], s_kv_r.at[l, c, 2 * k + i],
                      (seq_dst[k], p * 2 + h))

    def keys_in(l, c, k, j):
        return remote(kvo.at[j, c], kvb.at[l, c, seq_src[k], j], s_kv_s.at[c, 2 * k + j],
                      s_kv_r.at[l, c, 2 * k + j], (seq_dst[k], p * 2 + j))

    def mixed_out(c, k, j):
        return remote(ax.at[j, c], ab.at[c, v], s_at_s.at[c, 2 * k + j], s_at_r.at[c, 2 * k + i],
                      (s, var_dst[k] * 2 + j))

    def mixed_in(c, k, j):
        return remote(ax.at[j, c], ab.at[c, var_src[k] * 2 + j], s_at_s.at[c, 2 * k + j], s_at_r.at[c, 2 * k + j],
                      (s, var_dst[k] * 2 + j))

    def pool_products(blocks, mat):
        for q in range(8):
            sb = blocks[q][:, :64]
            blk = jnp.concatenate(
                [jnp.where(lane64 // 16 == n, sb, jnp.where(lane64 == 48 + n, 1.0, 0.0)) for n in range(3)], axis=0
            ).astype(BF16)
            kk = dot(blk, mat(q, pl.ds(0, 1024)))
            kb[q] = kk.astype(BF16)
            k2[q] = (kk * kk).astype(BF16)
            vv[q] = dot(blk, mat(q, pl.ds(1024, 1024))).astype(BF16)
        ss = dot_t(k2[...].reshape(768, 1024), hexp[...])
        qk = dot_t(kb[...].reshape(768, 1024), qexp[...])
        w = jnp.exp(qk * lax.rsqrt(ss * (1.0 / 64.0) + EPS_UNIT) * tvec)
        wb[...] = w.astype(BF16).reshape(8, 96, 128)

    def start_rows(pooled, step):
        row16 = lax.broadcasted_iota(jnp.int32, (16, 16), 1)
        lhot = jnp.where(row16 == lead[0] + step, 1.0, 0.0).astype(BF16)
        add = posv[...].astype(F32) + dot(lhot, leadt[...])
        own = dot(pooled.astype(BF16), aout[...]) + add
        for n in range(2):
            start_gather(n, own[8 * n : 8 * n + 8])

    pool_products(fsnd, lambda q, cols: m0[:, cols])
    for q in range(8):
        wx = dot(wb[q], hexp[...])
        nx = wx * vv[q].astype(F32)
        wq3 = wb[q].astype(F32)
        n0[:, q, :, pl.ds(0, 1024)] = (nx[0:32] + nx[32:64] + nx[64:96]).reshape(2, 16, 1024).astype(BF16)
        n0[:, q, :, pl.ds(1024, 128)] = (wq3[0:32] + wq3[32:64] + wq3[64:96]).reshape(2, 16, 128).astype(BF16)
    c0 = partner(n0.at[1 - i], p0r, 7)
    c0.start()
    for c in loads[6:12]:
        c.wait()
    loads[16].wait()
    c0.wait_recv()
    p0x[...] = (n0[i].astype(F32) + p0r[...].astype(F32)).astype(BF16)

    def pool_sums(k):
        return remote(p0x.at[var_dst[k]], p0b.at[k], s_p0_s.at[k], s_p0_r.at[k], var_dev(var_dst[k]))

    for k in range(7):
        pool_sums(k).start()
    wo_spread(0)
    for c in scalars[1:]:
        c.wait()
    tot = p0x[p].astype(F32)
    for k in (6, 5, 4, 3, 2, 1, 0):
        pool_sums(k).wait_recv()
        tot = tot + p0b[k].astype(F32)
    inv = 1.0 / tot[:, 1024:]
    inv_hi = inv.astype(BF16)
    inv_lo = (inv - inv_hi.astype(F32)).astype(BF16)
    start_rows(tot[:, :1024] * (dot(inv_hi, hexp[...]) + dot(inv_lo, hexp[...])), 0)
    c0.wait_send()
    for k in range(7):
        pool_sums(k).wait_send()
    for c in loads[12:16]:
        c.wait()
    for c in wcopies:
        c.wait()

    def step_body(step, carry):
        @pl.when(step == 1)
        def _():
            pool_products(st, lambda q, cols: mb[q, :, cols])
            num = jnp.zeros((32, 1024), F32)
            den = jnp.zeros((32, 1024), F32)
            for q in range(8):
                wx = dot(wb[q], hexp[...])
                nx = wx * vv[q].astype(F32)
                num = num + (nx[0:32] + nx[32:64] + nx[64:96])
                den = den + (wx[0:32] + wx[32:64] + wx[64:96])
            ndx[:, :, pl.ds(0, 1024)] = num.reshape(2, 16, 1024)
            ndx[:, :, pl.ds(1024, 1024)] = den.reshape(2, 16, 1024)
            c = partner(ndx.at[1 - i], ndr, 0)
            c.start()
            c.wait_recv()
            tot = ndx[i] + ndr[...]
            start_rows(tot[:, :1024] / tot[:, 1024:], 1)
            c.wait_send()

        def layer_body(l, carry):
            for n in range(2):
                for k in range(7):
                    gather(n, k, var_src[k]).wait_recv()
                x = layer_norm(xg[n].astype(F32).reshape(64, 1024), gains[l, pl.ds(0, 1), :]).astype(BF16)
                both = dot_t(x, wkv[l].reshape(256, 1024))
                for h in range(2):
                    kv = both[:, 128 * h : 128 * h + 128]
                    kq = jnp.where(left64, kv * kv, 0.0)
                    scale = lax.rsqrt(jnp.sum(kq, axis=-1, keepdims=True) * (1.0 / 64.0) + EPS_UNIT)
                    kvo[h, n] = (kv * jnp.where(left64, scale, 1.0)).astype(BF16)
                for k in range(7):
                    for h in range(2):
                        keys_out(l, n, k, h).start()
                partner(kvo.at[1 - i, n], kvb.at[l, n, s, i], 5 + n).start()
                kvb[l, n, s, i] = kvo[i, n]
                both = dot_t(x, wq[l].reshape(256, 1024))
                for h in range(2):
                    q = both[:, 128 * h : 128 * h + 128]
                    q = q * lax.rsqrt(jnp.sum(q * q, axis=-1, keepdims=True) * (1.0 / 64.0) + EPS_UNIT)
                    qx[h, n] = q.astype(BF16)
            partner(qx.at[1 - i], qb.at[i], 1).start()
            qb[i] = qx[i]

            @pl.when((step == 0) & (l == 0))
            def _():
                for k in (0, 1, 3, 5):
                    emb_copy(k, p).start()

            @pl.when((step == 0) & (l == 1))
            def _():
                for k in (2, 4, 6):
                    emb_copy(k, p).start()
                for k in range(7):
                    field_copy(k, p).start()

            @pl.when(step == 0)
            def _():
                for dz in (1, 2, 3):
                    wo_quarter(l, dz, True).wait_recv()
                wo_pass(l, i).start()

            for n in range(2):
                for k in range(7):
                    gather(n, k, p).wait_send()
            partner(qx.at[1 - i], qb.at[1 - i], 1).wait_recv()
            scale = temp[l] * (1.0 / 64.0)
            q = qb[...].reshape(256, 128)
            num = jnp.zeros((256, 128), F32)
            den = jnp.zeros((256, 128), F32)
            for n in range(2):
                for pair in ((7, 6), (5, 4), (3, 2), (1, 0)):
                    block = []
                    for k in pair:
                        if k == 7:
                            partner(kvo.at[1 - i, n], kvb.at[l, n, s, 1 - i], 5 + n).wait_recv()
                            block.append(kvb[l, n, s].reshape(128, 128))
                        else:
                            for j in range(2):
                                keys_in(l, n, k, j).wait_recv()
                            block.append(kvb[l, n, seq_src[k]].reshape(128, 128))
                    kv = jnp.concatenate(block, axis=0)
                    e = jnp.exp(dot_t(q, kv) * scale)
                    den = den + e[:, :128] + e[:, 128:]
                    num = num + dot(e.astype(BF16), kv)
            att = num / jnp.sum(den, axis=-1, keepdims=True)
            for n in range(2):
                for h in range(2):
                    r = 128 * h + 64 * n
                    ax[h, n] = jnp.where(
                        left64[:32], pltpu.roll(att[r : r + 32], 64, 1), att[r + 32 : r + 64]
                    ).astype(BF16)
                for k in range(7):
                    for j in range(2):
                        mixed_out(n, k, j).start()
                partner(ax.at[1 - i, n], ab.at[n, v], 2 + n).start()
                ab[n, v] = ax[i, n]
            @pl.when((step == 0) & (l == 0))
            def _():
                wo_spread(1)

            for n in range(2):
                for k in range(7):
                    for h in range(2):
                        keys_out(l, n, k, h).wait_send()
                partner(kvo.at[1 - i, n], kvb.at[l, n, s, i], 5 + n).wait_send()
            partner(qx.at[1 - i], qb.at[i], 1).wait_send()

            @pl.when(step == 0)
            def _():
                wo_pass(l, 1 - i).wait_recv()
                wo_pass(l, i).wait_send()
                for k in range(7):
                    wo_copy(l, k).wait_send()
                for dz in (1, 2, 3):
                    wo_quarter(l, dz, False).wait_send()

            @pl.when((step == 0) & (l == 1))
            def _():
                all_channels()

            for n in range(2):
                partner(ax.at[1 - i, n], ab.at[n, p * 2 + 1 - i], 2 + n).wait_recv()
                for k in range(7):
                    for j in range(2):
                        mixed_in(n, k, j).wait_recv()
                for q in range(8):
                    even, odd = ab[n, 2 * q].astype(F32), ab[n, 2 * q + 1].astype(F32)
                    cols = pl.ds(q * 128, 128)
                    at[n, pl.ds(0, 32), cols] = jnp.where(left64[:32], even, pltpu.roll(odd, 64, 1)).astype(BF16)
                    at[n, pl.ds(32, 32), cols] = jnp.where(left64[:32], pltpu.roll(even, 64, 1), odd).astype(BF16)
                rows = xg[n].astype(F32).reshape(64, 1024) + dot(at[n], wo[l].reshape(1024, 1024))
                rs[n] = rows.reshape(8, 8, 1024)
                x = layer_norm(rows, gains[l, pl.ds(1, 1), :]).astype(BF16)
                part = jnp.zeros((64, 1024), F32)
                for h in range(2):
                    hid = dot(x, wu[h, l])
                    hid = 0.5 * hid * (1.0 + lax.erf(hid * (0.5 ** 0.5)))
                    part = part + dot(hid.astype(BF16), wd[h, l])
                pb[n] = part.reshape(8, 8, 1024).astype(BF16)
                for k in range(7):
                    sums(n, k).start()

            for n in range(2):
                own = rs[n, p] + pb[n, p].astype(F32)
                for k in (6, 5, 4, 3, 2, 1, 0):
                    sums(n, k).wait_recv()
                    own = own + rsb[n, k].astype(F32)

                @pl.when(l < LAYERS - 1)
                def _(n=n, own=own):
                    start_gather(n, own)

                resid[pl.ds(8 * n, 8), :] = own
            for n in range(2):
                for k in range(7):
                    sums(n, k).wait_send()
                    for j in range(2):
                        mixed_out(n, k, j).wait_send()
                partner(ax.at[1 - i, n], ab.at[n, v], 2 + n).wait_send()
            return carry

        lax.fori_loop(0, LAYERS, layer_body, 0)
        fb[i] = layer_norm(resid[...], fgain[...]).astype(BF16)
        c = partner(fb.at[i], fb.at[i], 4)
        c.start()
        partner(fb.at[i], fb.at[1 - i], 4).wait_recv()
        fin = fb[...].reshape(32, 1024)
        for q in range(8):
            d = dot_t(fin, headp[q])
            st[q] = st[q] + d
            db[step, q] = d.astype(BF16)
        c.wait_send()
        for k in range(7):
            remote(db.at[step, var_dst[k]], dlr.at[step, p], s_d_s.at[step, k], s_d_r.at[step, k],
                   var_dev(var_dst[k])).start()
        dlr[step, p] = db[step, p]
        return carry

    lax.fori_loop(0, STEPS, step_body, 0)

    state = fields[:, 0, :]
    for step in range(STEPS):
        for k in range(7):
            c = remote(db.at[step, var_dst[k]], dlr.at[step, var_src[k]], s_d_s.at[step, k],
                       s_d_r.at[step, k], var_dev(var_dst[k]))
            c.wait_recv()
            c.wait_send()
        d = jnp.transpose(dlr[step].astype(F32).reshape(256, 128))
        state = state + d[:48]
        out[step] = state.reshape(48, 1, 256)


def per_device(
    fields, channel_ids, lead_index, embed_weight, var_table, agg_query, agg_kv, agg_out,
    agg_temp, pos_table, lead_table, norm_gain, qkv_weight, attn_temp, out_weight,
    up_weight, down_weight, final_gain, head_weight,
):
    vm = pl.BlockSpec(memory_space=pltpu.VMEM)
    hb = pl.BlockSpec(memory_space=pl.ANY)
    dma = pltpu.SemaphoreType.DMA
    V = pltpu.VMEM
    qkv_t = jnp.transpose(qkv_weight, (0, 2, 3, 1)).reshape(LAYERS, 192, 1024)
    head_t = jnp.transpose(head_weight, (1, 2, 0)).reshape(8, 2, 48, 1024)
    out = pl.pallas_call(
        kernel,
        out_shape=jax.ShapeDtypeStruct((STEPS, 48, 1, 256), F32),
        in_specs=[hb] * 19,
        out_specs=vm,
        scratch_shapes=[
            pltpu.SMEM((3,), jnp.int32),
            pltpu.SMEM((1,), jnp.int32),
            pltpu.SMEM((LAYERS,), F32),
            V((48, 1, 256), F32),
            V((48, 1024), BF16),
            V((16, 64), BF16),
            V((1, 16), F32),
            V((16, 1024), BF16),
            V((LAYERS, 2, 1024), F32),
            V((1, 1024), F32),
            V((1024, 2, 1024), BF16),
            V((LAYERS, 2, 128, 1024), BF16),
            V((LAYERS, 2, 128, 1024), BF16),
            V((LAYERS, 8, 2, 64, 1024), BF16),
            V((2, LAYERS, 1024, 256), BF16),
            V((2, LAYERS, 256, 1024), BF16),
            V((1024, 2048), BF16),
            V((1024, 1024), BF16),
            V((8, 128, 1024), BF16),
            V((16, 1024), BF16),
            V((8, 32, 128), F32),
            V((8, 32, 128), F32),
            V((8, 48, 1024), BF16),
            V((8, 64, 2048), BF16),
            V((64, 2048), BF16),
            V((2, 8, 16, 1152), BF16),
            V((8, 16, 1152), BF16),
            V((8, 16, 1152), BF16),
            V((7, 16, 1152), BF16),
            V((8, 96, 1024), BF16),
            V((8, 96, 1024), BF16),
            V((8, 96, 1024), BF16),
            V((8, 96, 128), BF16),
            V((2, 16, 2048), F32),
            V((16, 2048), F32),
            V((128, 1024), BF16),
            V((128, 1024), BF16),
            V((16, 1024), F32),
            V((2, 8, 8, 1024), BF16),
            V((2, 8, 8, 1024), BF16),
            V((2, 7, 8, 1024), BF16),
            V((2, 2, 64, 128), BF16),
            V((2, 2, 64, 128), BF16),
            V((LAYERS, 2, 8, 2, 64, 128), BF16),
            V((2, 2, 64, 128), BF16),
            V((2, 2, 32, 128), BF16),
            V((2, 16, 32, 128), BF16),
            V((2, 64, 1024), BF16),
            V((2, 8, 8, 1024), F32),
            V((2, 16, 1024), BF16),
            V((STEPS, 8, 32, 128), BF16),
            V((STEPS, 8, 32, 128), BF16),
            dma((17,)),
            dma((3,)),
            dma((5,)), dma((5,)),
            dma((7,)), dma((7,)),
            dma((7,)), dma((7,)),
            dma((2, 7)), dma((2, 7)),
            dma((2, 7)), dma((2, 7)),
            dma((2, 14)), dma((LAYERS, 2, 14)),
            dma((8,)), dma((8,)),
            dma((STEPS, 7)), dma((STEPS, 7)),
            dma((2, 14)), dma((2, 14)),
            dma((LAYERS, 7)), dma((LAYERS, 7)),
            dma((LAYERS, 3)), dma((LAYERS, 3)),
            dma((LAYERS,)), dma((LAYERS,)),
            dma((7,)), dma((7,)),
        ],
        compiler_params=pltpu.CompilerParams(
            collective_id=0, has_side_effects=True, vmem_limit_bytes=60 * 1024 * 1024
        ),
        name="rollout",
    )(
        channel_ids,
        lead_index,
        attn_temp.reshape(LAYERS),
        fields.reshape(48, 1, 256),
        embed_weight.reshape(48, 1024),
        var_table,
        agg_query,
        agg_kv,
        agg_out,
        agg_temp.reshape(1, 16),
        pos_table,
        lead_table,
        norm_gain,
        qkv_t,
        out_weight.reshape(LAYERS, 64, 1024),
        up_weight,
        down_weight,
        final_gain.reshape(1, 1024),
        head_t,
    )
    return out.reshape(STEPS, 3, 16, 1, 256)


def solution(mesh):
    return jax.shard_map(
        per_device,
        mesh=mesh,
        in_specs=(
            P("var", None, None, "seq"),
            P("var"),
            P(),
            P("var", None, None),
            P(),
            P(),
            P(),
            P(),
            P(),
            P("seq", None),
            P(),
            P(),
            P(None, None, "var", None),
            P(None, "var"),
            P(None, "var", None, None),
            P(None, None, "var"),
            P(None, "var", None),
            P(),
            P(),
        ),
        out_specs=P(None, "var", None, None, "seq"),
        check_vma=False,
    )
```
